128 devices in a mesh: omega: 16 (over x, z_hi, core), row: 8 (over y, z_lo).
Axes of the slice: x: 4, y: 4, z: 4 (z_hi: 2, z_lo: 2; z = z_hi * 2 + z_lo), core: 2. Of those that a mesh axis runs over, the one named last changes fastest.
Arguments:
- frames: float32 [256, 512, 1024], P('omega', 'row'), may hold values from -6 to 6
- thresholds: int32 [512], P('row'), may hold values from 0 to 31
- spot_boxes: int32 [3, 4096], P(None, ('omega', 'row')), may hold values from -1 to 1023, as said below
Outputs:
- peak_weight: float32 [256, 512, 1024], P('omega', 'row')
- moments: float32 [4, 4096], P(None, ('omega', 'row'))
The draws below stay inside these ranges and needn't reach their ends.
Inputs may be any that keep to these rules, and one draw needn't show every extreme that they name: `spot_boxes`: slot block d of 32 slots (d = omega index * the number of row indices + row index) lists boxes that lie wholly inside the frames and rows of that device; its live boxes fill the leading slots, each block has 1 to 32 of them, and one block has 32; empty slots hold -1 in all three entries.
All inputs are finite; a program needn't handle non-finite values.
Results may differ from the reference program's by a relative error of at most 0.0003.
Values sent between devices are 32-bit elements; how exact they have to be, the bound alone decides.
A program may use at most 64 MiB of HBM per device.

```python
import jax
import jax.numpy as jnp
from jax import lax

FR_DEV = 16
ROWS_DEV = 64
COLS = 1024
CAP = 32
BW = 4
BOX_F = 8
BOX_R = 16
BOX_C = 16
FRAMES = 256
ROWS = 512
N_OMEGA = 16
N_ROW = 8


def draw_spot_boxes(key, part):
    blocks = N_OMEGA * N_ROW
    key_busy = jax.random.fold_in(key, 11)
    key_live = jax.random.fold_in(key, 12)
    key_frame = jax.random.fold_in(key, 13)
    key_row = jax.random.fold_in(key, 14)
    key_column = jax.random.fold_in(key, 15)
    block_ids = jnp.arange(blocks)
    omega_ids = block_ids // N_ROW
    row_ids = block_ids % N_ROW
    busiest = jax.random.randint(key_busy, (), 0, blocks)
    live = jax.random.randint(key_live, (blocks,), 1, CAP // 2 + 1)
    live = jnp.where(block_ids == busiest, CAP, live)
    first = jax.random.randint(key_frame, (blocks, CAP), 0, FR_DEV - BOX_F + 1) + omega_ids[:, None] * FR_DEV
    second = jax.random.randint(key_row, (blocks, CAP), 0, ROWS_DEV - BOX_R + 1) + row_ids[:, None] * ROWS_DEV
    third = jax.random.randint(key_column, (blocks, CAP), 0, COLS - BOX_C + 1)
    alive = jnp.arange(CAP)[None, :] < live[:, None]
    stacked = jnp.stack([first, second, third])
    stacked = jnp.where(alive[None], stacked, -1)
    return stacked.reshape(3, blocks * CAP).astype(jnp.int32)


def plant(result, rng, least, high):
    place = [jax.random.randint(jax.random.fold_in(rng, axis), (), 0, length) for axis, length in enumerate(result.shape)]
    longest = result.shape.index(max(result.shape))
    neighbour = place[:longest] + [(place[longest] + 1) % result.shape[longest]] + place[longest + 1:]
    return result.at[tuple(place)].set(least).at[tuple(neighbour)].set(high)


def level_of(key, shape, pieces, least, largest):
    factor_of, own = 1.0, jax.random.fold_in(key, 6)
    for dim, blocks in pieces:
        draws = jnp.exp(jax.random.uniform(jax.random.fold_in(own, dim), (blocks,), jnp.float32, least / len(pieces), largest / len(pieces)))
        factor_of = factor_of * jnp.repeat(draws, shape[dim] // blocks).reshape([-1 if axis == dim else 1 for axis in range(len(shape))])
    return factor_of


def noise(rng, extent, width, bound, pieces=(), held_as=jnp.bfloat16):
    values = width * jax.random.normal(rng, extent, jnp.float32)
    if pieces:
        values = values * level_of(rng, extent, pieces, -0.22, 0.18)
    return jnp.clip(values, -bound, bound).astype(held_as)


def setup_inputs(seed: int = 0) -> dict:
    key_of = jax.random.split(jax.random.key(seed), 4)
    frames = noise(key_of[0], (FRAMES, ROWS, COLS), 1.0, 6.0, ((0, 16), (1, 8)), jnp.float32)
    thresholds = plant(jax.random.randint(key_of[1], (ROWS,), 0, 32), jax.random.fold_in(key_of[1], 1), 0, 31).astype(jnp.int32)
    spot_boxes = draw_spot_boxes(jax.random.fold_in(key_of[3], 71), 0)
    return {"frames": frames, "thresholds": thresholds, "spot_boxes": spot_boxes}


SHARP = 8.0


def offsets_table(length):
    steps = jnp.arange(length).astype(jnp.float32)
    half = (length - 1) / 2.0
    return (steps - half) / half


def box_stats(weight, column):
    live = column[0] >= 0
    first = jnp.maximum(column[0], 0).astype(jnp.int32)
    second = jnp.maximum(column[1], 0).astype(jnp.int32)
    third = jnp.maximum(column[2], 0).astype(jnp.int32)
    patch = lax.dynamic_slice(weight, (first, second, third), (BOX_F, BOX_R, BOX_C))
    frame_off = offsets_table(BOX_F)[:, None, None]
    row_off = offsets_table(BOX_R)[None, :, None]
    column_off = offsets_table(BOX_C)[None, None, :]
    stats = jnp.stack([jnp.mean(patch), jnp.mean(patch * frame_off), jnp.mean(patch * row_off), jnp.mean(patch * column_off)])
    return jnp.where(live, stats, jnp.zeros_like(stats))


def one_frame(frames, level, index):
    reach = BW + 2
    span = 2 * BW + 1
    picks = ((jnp.arange(2 * reach + 1).astype(jnp.int32) - reach + index) % FRAMES).astype(jnp.int32)
    window = jnp.take(frames, picks, axis=0)
    total = window[0:5]
    for offset in range(1, span):
        total = total + window[offset:offset + 5]
    corrected = window[BW:BW + 5] - total / span
    smooth = (corrected[:-2] + 2.0 * corrected[1:-1] + corrected[2:]) * 0.25
    padded = jnp.pad(smooth, ((0, 0), (1, 1), (0, 0)))
    smooth = (padded[:, :-2] + 2.0 * padded[:, 1:-1] + padded[:, 2:]) * 0.25
    padded = jnp.pad(smooth, ((0, 0), (0, 0), (1, 1)))
    smooth = (padded[:, :, :-2] + 2.0 * padded[:, :, 1:-1] + padded[:, :, 2:]) * 0.25
    highest = jnp.maximum(jnp.maximum(smooth[0], smooth[1]), smooth[2])
    padded = jnp.pad(highest, ((1, 1), (0, 0)), mode="edge")
    highest = jnp.maximum(jnp.maximum(padded[:-2], padded[1:-1]), padded[2:])
    padded = jnp.pad(highest, ((0, 0), (1, 1)), mode="edge")
    highest = jnp.maximum(jnp.maximum(padded[:, :-2], padded[:, 1:-1]), padded[:, 2:])
    centre = smooth[1]
    return jnp.exp(SHARP * (centre - highest)) * jnp.maximum(centre - level[:, None], 0.0)


def reference(frames, thresholds, spot_boxes):
    level = thresholds.astype(jnp.float32) / 64.0
    weight = lax.map(lambda index: one_frame(frames, level, index), jnp.arange(FRAMES).astype(jnp.int32))
    stats = lax.map(lambda column: box_stats(weight, column), spot_boxes.T)
    return weight, stats.T
```

```python
import functools

import jax
import jax.numpy as jnp
from jax import lax
from jax.experimental import pallas as pl
from jax.experimental.pallas import tpu as pltpu
from jax.sharding import PartitionSpec as P

BW = 4
REACH = BW + 2
BOX_F = 8
BOX_R = 16
BOX_C = 16
SHARP = 8.0
LOG2E = 1.4426950408889634
BIG = 3.0e38
LANES = 128
DEPTH = 3
LATE = 4
MESH = pl.DeviceIdType.MESH


def spread_kernel(n_omega, n_row, frames, thresholds, weight, x, first, second, smooth, wide, level, outgoing, incoming, load_sem, send_sem, recv_sem, row_send, row_recv):
    depth, rows = (frames.shape[0], frames.shape[1])
    tiles = frames.shape[2] // LANES
    groups = rows // 8
    planes = depth + 2
    omega, row = (lax.axis_index("omega"), lax.axis_index("row"))
    after, before = (lax.rem(omega + 1, n_omega), lax.rem(omega + n_omega - 1, n_omega))
    has_upper, has_lower = (row > 0, row < n_row - 1)

    def load(t):
        return pltpu.make_async_copy(frames.at[:, :, pl.ds(t * LANES, LANES)], x.at[pl.ds(REACH, depth), t], load_sem.at[t])

    for t in range(tiles):
        load(t).start()

    barrier = pltpu.get_barrier_semaphore()
    for neighbour in (before, after):
        pl.semaphore_signal(barrier, inc=1, device_id=(neighbour, row), device_id_type=MESH)

    @pl.when(has_upper)
    def _():
        pl.semaphore_signal(barrier, inc=1, device_id=(omega, row - 1), device_id_type=MESH)

    @pl.when(has_lower)
    def _():
        pl.semaphore_signal(barrier, inc=1, device_id=(omega, row + 1), device_id_type=MESH)

    sub = lax.broadcasted_iota(jnp.int32, (8, LANES), 0)
    lane = lax.broadcasted_iota(jnp.int32, (8, LANES), 1)
    for g in range(groups):
        tile = jnp.full((8, LANES), thresholds[g * 8].astype(jnp.float32))
        for j in range(1, 8):
            tile = jnp.where(sub == j, thresholds[g * 8 + j].astype(jnp.float32), tile)
        level[g * 8 : g * 8 + 8, :] = tile
    blank = jnp.zeros((rows + 8, LANES), jnp.float32)
    for i in range(planes):
        second[i, 0] = blank
        second[i, tiles + 1] = blank

    def piece(start, chunk):
        planes_of = pl.ds(start, REACH)
        if isinstance(chunk, int) and chunk < 2:
            return x.at[planes_of, :, pl.ds(0 if chunk == 0 else rows - 8, 8), :]
        return x.at[planes_of, chunk - 2, pl.ds(8, rows - 16), :]

    def copies(chunk):
        to_before = pltpu.make_async_remote_copy(
            src_ref=piece(REACH, chunk), dst_ref=piece(REACH + depth, chunk), send_sem=send_sem.at[0, chunk], recv_sem=recv_sem.at[0, chunk], device_id=(before, row), device_id_type=MESH
        )
        to_after = pltpu.make_async_remote_copy(
            src_ref=piece(depth, chunk), dst_ref=piece(0, chunk), send_sem=send_sem.at[1, chunk], recv_sem=recv_sem.at[1, chunk], device_id=(after, row), device_id_type=MESH
        )
        return (to_before, to_after)

    def row_copy(side):
        return pltpu.make_async_remote_copy(
            src_ref=outgoing.at[side], dst_ref=incoming.at[side], send_sem=row_send.at[side], recv_sem=row_recv.at[side], device_id=(omega, row - 1 if side == 0 else row + 1), device_id_type=MESH
        )

    for t in range(tiles):
        load(t).wait()
    pl.semaphore_wait(barrier, 2 + has_upper.astype(jnp.int32) + has_lower.astype(jnp.int32))

    def issue(chunk):
        for copy in copies(chunk):
            copy.start()

    def arrive(chunk):
        for copy in copies(chunk):
            copy.wait_recv()
        for copy in copies(chunk):
            copy.wait_send()

    def frame_stage(t, start):
        v = [x[j, t, pl.ds(start, 8), :] for j in range(depth + 2 * REACH)]
        s2 = [v[j] + v[j + 1] for j in range(len(v) - 1)]
        s4 = [s2[j] + s2[j + 2] for j in range(len(s2) - 2)]
        s8 = [s4[j] + s4[j + 4] for j in range(len(s4) - 4)]
        c = [v[j + BW] - (s8[j] + v[j + 2 * BW]) * (1.0 / (2 * BW + 1)) for j in range(depth + 4)]
        p = [c[j] + c[j + 1] for j in range(depth + 3)]
        for i in range(planes):
            first[i, t, pl.ds(start + 8, 8), :] = p[i] + p[i + 1]

    def row_stage(t):
        def body(k, carry):
            for i in range(planes):
                up = first[i, t, pl.ds(8 * k + 6, 8), :]
                mid = first[i, t, pl.ds(8 * k + 7, 8), :]
                down = first[i, t, pl.ds(8 * k + 8, 8), :]
                second[i, t + 1, pl.ds(pl.multiple_of(8 * k, 8), 8), :] = (up + down) + (mid + mid)
            return carry

        lax.fori_loop(0, groups + 1, body, 0)

    def column_stage(t):
        left_edge, right_edge = (lane == 0, lane == LANES - 1)
        left_half = lane >= LANES // 2
        low = jnp.where(t == 0, -BIG, BIG)
        high = jnp.where(t == tiles - 1, -BIG, BIG)
        bound = jnp.where(left_half, low, high)

        def body(k, carry):
            at = pl.ds(pl.multiple_of(8 * k, 8), 8)
            for i in range(planes):
                a, b, c = (second[i, t, at, :], second[i, t + 1, at, :], second[i, t + 2, at, :])
                w = jnp.where(left_half, a, c)
                to_right = pltpu.roll(jnp.where(right_edge, a, b), 1, 1)
                to_left = pltpu.roll(jnp.where(left_edge, c, b), LANES - 1, 1)
                value = (to_right + to_left) + (b + b)
                w_right = pltpu.roll(jnp.where(right_edge, b, w), 1, 1)
                w_left = pltpu.roll(jnp.where(left_edge, b, w), LANES - 1, 1)
                beside = jnp.minimum((w_right + w_left) + (w + w), bound)
                from_left = pltpu.roll(jnp.where(right_edge, beside, value), 1, 1)
                from_right = pltpu.roll(jnp.where(left_edge, beside, value), LANES - 1, 1)
                wide[i, at, :] = jnp.maximum(jnp.maximum(from_left, from_right), value)
                if 0 < i < planes - 1:
                    smooth[i - 1, at, :] = value
            return carry

        lax.fori_loop(0, groups + 1, body, 0)

        @pl.when(jnp.logical_not(has_upper))
        def _():
            for i in range(planes):
                wide[i, 0:1, :] = jnp.full((1, LANES), -BIG)

        @pl.when(jnp.logical_not(has_lower))
        def _():
            for i in range(planes):
                wide[i, rows + 1 : rows + 2, :] = jnp.full((1, LANES), -BIG)

    def weight_stage(t):
        def body(g, carry):
            start = pl.multiple_of(8 * g, 8)
            limit = level[pl.ds(start, 8), :]
            tall = []
            for i in range(planes):
                up = wide[i, pl.ds(8 * g, 8), :]
                mid = wide[i, pl.ds(8 * g + 1, 8), :]
                down = wide[i, pl.ds(8 * g + 2, 8), :]
                tall.append(jnp.maximum(jnp.maximum(up, down), mid))
                if i >= 2:
                    highest = jnp.maximum(jnp.maximum(tall[i - 2], tall[i - 1]), tall[i])
                    value = smooth[i - 2, pl.ds(8 * g + 1, 8), :]
                    sharp = jnp.exp2((value - highest) * (SHARP * LOG2E / 64.0))
                    weight[i - 2, t, pl.ds(start, 8), :] = sharp * (jnp.maximum(value - limit, 0.0) * (1.0 / 64.0))
            return carry

        lax.fori_loop(0, groups, body, 0)

    def finish(t):
        column_stage(t)
        weight_stage(t)

    for chunk in range(DEPTH):
        issue(chunk)

    def edge(side):
        arrive(side)
        issue(side + DEPTH)
        start = 0 if side == 0 else rows - 8

        def body(t, carry):
            frame_stage(t, start)
            for i in range(planes):
                outgoing[side, pl.ds((i * tiles + t) * 2, 2), :] = first[i, t, pl.ds(8 if side == 0 else rows + 6, 2), :]
            return carry

        lax.fori_loop(0, tiles, body, 0)

        @pl.when(has_upper if side == 0 else has_lower)
        def _():
            row_copy(side).start()

    edge(0)
    edge(1)

    def take(t):
        arrive(t + 2)

        @pl.when(t + 2 + DEPTH < tiles + 2)
        def _():
            issue(t + 2 + DEPTH)

        def body(g, carry):
            frame_stage(t, pl.multiple_of(8 * g, 8))
            return carry

        lax.fori_loop(1, groups - 1, body, 0)

    def early(t, carry):
        take(t)
        return carry

    lax.fori_loop(0, LATE + 1, early, 0)

    for side in range(2):
        place = rows + 8 if side == 0 else 6
        there = has_lower if side == 0 else has_upper

        @pl.when(there)
        def _():
            row_copy(side).wait_recv()

            def body(t, carry):
                for i in range(planes):
                    first[i, t, pl.ds(place, 2), :] = incoming[side, pl.ds((i * tiles + t) * 2, 2), :]
                return carry

            lax.fori_loop(0, tiles, body, 0)

        @pl.when(jnp.logical_not(there))
        def _():
            def body(t, carry):
                for i in range(planes):
                    first[i, t, pl.ds(place, 2), :] = jnp.zeros((2, LANES), jnp.float32)
                return carry

            lax.fori_loop(0, tiles, body, 0)

    row_stage(0)

    def catch_up(t, carry):
        row_stage(t + 1)
        finish(t)
        return carry

    lax.fori_loop(0, LATE, catch_up, 0)

    def late(t, carry):
        take(t)
        row_stage(t)
        finish(t - 1)
        return carry

    lax.fori_loop(LATE + 1, tiles, late, 0)
    finish(tiles - 1)

    for side in range(2):

        @pl.when(has_upper if side == 0 else has_lower)
        def _():
            row_copy(side).wait_send()


def moments_kernel(boxes, weight, out, moments, parts, sem):
    depth, tiles, rows = weight.shape[0:3]
    slots = boxes.shape[1]

    def store(t):
        return pltpu.make_async_copy(weight.at[:, t], out.at[:, :, pl.ds(t * LANES, LANES)], sem.at[t])

    for t in range(tiles):
        store(t).start()
    frame_base = lax.axis_index("omega") * depth
    row_base = lax.axis_index("row") * rows
    sub = lax.broadcasted_iota(jnp.int32, (8, LANES), 0)
    lane = lax.broadcasted_iota(jnp.int32, (8, LANES), 1)
    half_f, half_r, half_c = ((BOX_F - 1) / 2.0, (BOX_R - 1) / 2.0, (BOX_C - 1) / 2.0)
    u_row = [((sub + 8 * j).astype(jnp.float32) - half_r) / half_r for j in range(2)]

    def box(b, carry):
        live = boxes[0, b] >= 0

        @pl.when(live)
        def _():
            f0 = boxes[0, b] - frame_base
            r0 = boxes[1, b] - row_base
            c0 = boxes[2, b]
            totals = None
            for side in range(2):
                tile = jnp.minimum(c0 // LANES + side, tiles - 1)
                distance = lane - (lax.rem(c0, LANES) - side * LANES)
                inside = (distance >= 0) & (distance < BOX_C)
                u_column = (distance.astype(jnp.float32) - half_c) / half_c
                plain = [None, None]
                framed = [None, None]
                for j in range(2):
                    for i in range(BOX_F):
                        w = weight[f0 + i, tile, pl.ds(r0 + 8 * j, 8), :]
                        m = w * ((i - half_f) / half_f)
                        plain[j] = w if i == 0 else plain[j] + w
                        framed[j] = m if i == 0 else framed[j] + m
                everything = plain[0] + plain[1]
                stats = [everything, framed[0] + framed[1], plain[0] * u_row[0] + plain[1] * u_row[1], everything * u_column]
                stats = [jnp.where(inside, s, 0.0) for s in stats]
                totals = stats if side == 0 else [p + q for p, q in zip(totals, stats)]
            for s in range(4):
                parts[s, pl.ds(pl.multiple_of(b * 8, 8), 8), :] = totals[s]

        @pl.when(jnp.logical_not(live))
        def _():
            for s in range(4):
                parts[s, pl.ds(pl.multiple_of(b * 8, 8), 8), :] = jnp.zeros((8, LANES), jnp.float32)

        return carry

    lax.fori_loop(0, slots, box, 0)
    ones = jnp.ones((8, LANES), jnp.float32)
    lines = []
    for s in range(4):
        total = parts[s, pl.ds(0, slots, stride=8), :]
        for j in range(1, 8):
            total = total + parts[s, pl.ds(j, slots, stride=8), :]
        sums = lax.dot_general(ones, total, (((1,), (1,)), ((), ())), precision=lax.Precision.HIGHEST, preferred_element_type=jnp.float32)
        lines.append(sums[0:1, :])
    moments[...] = jnp.concatenate(lines, axis=0) * (1.0 / (BOX_F * BOX_R * BOX_C))
    for t in range(tiles):
        store(t).wait()


def on_device(n_omega, n_row, frames, thresholds, spot_boxes):
    depth, rows, columns = frames.shape
    tiles = columns // LANES
    planes = depth + 2
    slots = spot_boxes.shape[1]
    vmem = functools.partial(pl.BlockSpec, memory_space=pltpu.VMEM)
    smem = functools.partial(pl.BlockSpec, memory_space=pltpu.SMEM)
    anywhere = functools.partial(pl.BlockSpec, memory_space=pl.ANY)
    weight = pl.pallas_call(
        functools.partial(spread_kernel, n_omega, n_row),
        out_shape=pltpu.VMEM((depth, tiles, rows, LANES), jnp.float32),
        in_specs=[pl.BlockSpec(memory_space=pltpu.HBM), smem()],
        out_specs=vmem(),
        scratch_shapes=[
            pltpu.VMEM((depth + 2 * REACH, tiles, rows, LANES), jnp.float32),
            pltpu.VMEM((planes, tiles, rows + 16, LANES), jnp.float32),
            pltpu.VMEM((planes, tiles + 2, rows + 8, LANES), jnp.float32),
            pltpu.VMEM((depth, rows + 8, LANES), jnp.float32),
            pltpu.VMEM((planes, rows + 8, LANES), jnp.float32),
            pltpu.VMEM((rows, LANES), jnp.float32),
            pltpu.VMEM((2, planes * tiles * 2, LANES), jnp.float32),
            pltpu.VMEM((2, planes * tiles * 2, LANES), jnp.float32),
            pltpu.SemaphoreType.DMA((tiles,)),
            pltpu.SemaphoreType.DMA((2, tiles + 2)),
            pltpu.SemaphoreType.DMA((2, tiles + 2)),
            pltpu.SemaphoreType.DMA((2,)),
            pltpu.SemaphoreType.DMA((2,)),
        ],
        compiler_params=pltpu.CompilerParams(collective_id=0, has_side_effects=True, vmem_limit_bytes=32 << 20),
        name="spread",
    )(frames, thresholds)
    return pl.pallas_call(
        moments_kernel,
        out_shape=(jax.ShapeDtypeStruct(frames.shape, jnp.float32), jax.ShapeDtypeStruct((4, slots), jnp.float32)),
        in_specs=[smem(), vmem()],
        out_specs=(anywhere(), vmem()),
        scratch_shapes=[pltpu.VMEM((4, slots * 8, LANES), jnp.float32), pltpu.SemaphoreType.DMA((tiles,))],
        compiler_params=pltpu.CompilerParams(vmem_limit_bytes=8 << 20),
        name="moments",
    )(spot_boxes, weight)


def solution(mesh):
    return jax.shard_map(
        functools.partial(on_device, mesh.shape["omega"], mesh.shape["row"]),
        mesh=mesh,
        in_specs=(P("omega", "row", None), P("row"), P(None, ("omega", "row"))),
        out_specs=(P("omega", "row", None), P(None, ("omega", "row"))),
        check_vma=False,
    )
```

```python
import functools

import jax
import jax.numpy as jnp
from jax import lax
from jax.experimental import pallas as pl
from jax.experimental.pallas import tpu as pltpu
from jax.sharding import PartitionSpec as P

BW = 4
REACH = BW + 2
BOX_F = 8
BOX_R = 16
BOX_C = 16
SHARP = 8.0
LOG2E = 1.4426950408889634
BIG = 3.0e38
LANES = 128
DEPTH = 3
LATE = 4
MESH = pl.DeviceIdType.MESH


def spread_kernel(n_omega, n_row, frames, limits, weight, thresholds, x, first, second, smooth, wide, level, outgoing, incoming, limit_sem, load_sem, send_sem, recv_sem, row_send, row_recv):
    depth, rows = (frames.shape[0], frames.shape[1])
    tiles = frames.shape[2] // LANES
    groups = rows // 8
    planes = depth + 2
    omega, row = (lax.axis_index("omega"), lax.axis_index("row"))
    after, before = (lax.rem(omega + 1, n_omega), lax.rem(omega + n_omega - 1, n_omega))
    has_upper, has_lower = (row > 0, row < n_row - 1)

    def load(t):
        return pltpu.make_async_copy(frames.at[:, :, pl.ds(t * LANES, LANES)], x.at[pl.ds(REACH, depth), t], load_sem.at[t])

    limits_copy = pltpu.make_async_copy(limits, thresholds, limit_sem)
    limits_copy.start()
    for t in range(tiles):
        load(t).start()

    barrier = pltpu.get_barrier_semaphore()
    for neighbour in (before, after):
        pl.semaphore_signal(barrier, inc=1, device_id=(neighbour, row), device_id_type=MESH)

    @pl.when(has_upper)
    def _():
        pl.semaphore_signal(barrier, inc=1, device_id=(omega, row - 1), device_id_type=MESH)

    @pl.when(has_lower)
    def _():
        pl.semaphore_signal(barrier, inc=1, device_id=(omega, row + 1), device_id_type=MESH)

    sub = lax.broadcasted_iota(jnp.int32, (8, LANES), 0)
    lane = lax.broadcasted_iota(jnp.int32, (8, LANES), 1)
    limits_copy.wait()
    for g in range(groups):
        tile = jnp.full((8, LANES), thresholds[g * 8].astype(jnp.float32))
        for j in range(1, 8):
            tile = jnp.where(sub == j, thresholds[g * 8 + j].astype(jnp.float32), tile)
        level[g * 8 : g * 8 + 8, :] = tile
    blank = jnp.zeros((rows + 8, LANES), jnp.float32)
    for i in range(planes):
        second[i, 0] = blank
        second[i, tiles + 1] = blank

    def piece(start, chunk):
        planes_of = pl.ds(start, REACH)
        if isinstance(chunk, int) and chunk < 2:
            return x.at[planes_of, :, pl.ds(0 if chunk == 0 else rows - 8, 8), :]
        return x.at[planes_of, chunk - 2, pl.ds(8, rows - 16), :]

    def copies(chunk):
        to_before = pltpu.make_async_remote_copy(
            src_ref=piece(REACH, chunk), dst_ref=piece(REACH + depth, chunk), send_sem=send_sem.at[0, chunk], recv_sem=recv_sem.at[0, chunk], device_id=(before, row), device_id_type=MESH
        )
        to_after = pltpu.make_async_remote_copy(
            src_ref=piece(depth, chunk), dst_ref=piece(0, chunk), send_sem=send_sem.at[1, chunk], recv_sem=recv_sem.at[1, chunk], device_id=(after, row), device_id_type=MESH
        )
        return (to_before, to_after)

    def row_copy(side):
        return pltpu.make_async_remote_copy(
            src_ref=outgoing.at[side], dst_ref=incoming.at[side], send_sem=row_send.at[side], recv_sem=row_recv.at[side], device_id=(omega, row - 1 if side == 0 else row + 1), device_id_type=MESH
        )

    for t in range(tiles):
        load(t).wait()
    pl.semaphore_wait(barrier, 2 + has_upper.astype(jnp.int32) + has_lower.astype(jnp.int32))

    def issue(chunk):
        for copy in copies(chunk):
            copy.start()

    def arrive(chunk):
        for copy in copies(chunk):
            copy.wait_recv()
        for copy in copies(chunk):
            copy.wait_send()

    def frame_stage(t, start):
        v = [x[j, t, pl.ds(start, 8), :] for j in range(depth + 2 * REACH)]
        s2 = [v[j] + v[j + 1] for j in range(len(v) - 1)]
        s4 = [s2[j] + s2[j + 2] for j in range(len(s2) - 2)]
        s8 = [s4[j] + s4[j + 4] for j in range(len(s4) - 4)]
        c = [v[j + BW] - (s8[j] + v[j + 2 * BW]) * (1.0 / (2 * BW + 1)) for j in range(depth + 4)]
        p = [c[j] + c[j + 1] for j in range(depth + 3)]
        for i in range(planes):
            first[i, t, pl.ds(start + 8, 8), :] = p[i] + p[i + 1]

    def row_stage(t):
        def body(k, carry):
            for i in range(planes):
                up = first[i, t, pl.ds(8 * k + 6, 8), :]
                mid = first[i, t, pl.ds(8 * k + 7, 8), :]
                down = first[i, t, pl.ds(8 * k + 8, 8), :]
                second[i, t + 1, pl.ds(pl.multiple_of(8 * k, 8), 8), :] = (up + down) + (mid + mid)
            return carry

        lax.fori_loop(0, groups + 1, body, 0)

    def column_stage(t):
        left_edge, right_edge = (lane == 0, lane == LANES - 1)
        left_half = lane >= LANES // 2
        low = jnp.where(t == 0, -BIG, BIG)
        high = jnp.where(t == tiles - 1, -BIG, BIG)
        bound = jnp.where(left_half, low, high)

        def body(k, carry):
            at = pl.ds(pl.multiple_of(8 * k, 8), 8)
            for i in range(planes):
                a, b, c = (second[i, t, at, :], second[i, t + 1, at, :], second[i, t + 2, at, :])
                w = jnp.where(left_half, a, c)
                to_right = pltpu.roll(jnp.where(right_edge, a, b), 1, 1)
                to_left = pltpu.roll(jnp.where(left_edge, c, b), LANES - 1, 1)
                value = (to_right + to_left) + (b + b)
                w_right = pltpu.roll(jnp.where(right_edge, b, w), 1, 1)
                w_left = pltpu.roll(jnp.where(left_edge, b, w), LANES - 1, 1)
                beside = jnp.minimum((w_right + w_left) + (w + w), bound)
                from_left = pltpu.roll(jnp.where(right_edge, beside, value), 1, 1)
                from_right = pltpu.roll(jnp.where(left_edge, beside, value), LANES - 1, 1)
                wide[i, at, :] = jnp.maximum(jnp.maximum(from_left, from_right), value)
                if 0 < i < planes - 1:
                    smooth[i - 1, at, :] = value
            return carry

        lax.fori_loop(0, groups + 1, body, 0)

        @pl.when(jnp.logical_not(has_upper))
        def _():
            for i in range(planes):
                wide[i, 0:1, :] = jnp.full((1, LANES), -BIG)

        @pl.when(jnp.logical_not(has_lower))
        def _():
            for i in range(planes):
                wide[i, rows + 1 : rows + 2, :] = jnp.full((1, LANES), -BIG)

    def weight_stage(t):
        def body(g, carry):
            start = pl.multiple_of(8 * g, 8)
            limit = level[pl.ds(start, 8), :]
            tall = []
            for i in range(planes):
                up = wide[i, pl.ds(8 * g, 8), :]
                mid = wide[i, pl.ds(8 * g + 1, 8), :]
                down = wide[i, pl.ds(8 * g + 2, 8), :]
                tall.append(jnp.maximum(jnp.maximum(up, down), mid))
                if i >= 2:
                    highest = jnp.maximum(jnp.maximum(tall[i - 2], tall[i - 1]), tall[i])
                    value = smooth[i - 2, pl.ds(8 * g + 1, 8), :]
                    sharp = jnp.exp2((value - highest) * (SHARP * LOG2E / 64.0))
                    weight[i - 2, t, pl.ds(start, 8), :] = sharp * (jnp.maximum(value - limit, 0.0) * (1.0 / 64.0))
            return carry

        lax.fori_loop(0, groups, body, 0)

    def finish(t):
        column_stage(t)
        weight_stage(t)

    for chunk in range(DEPTH):
        issue(chunk)

    def edge(side):
        arrive(side)
        issue(side + DEPTH)
        start = 0 if side == 0 else rows - 8

        def body(t, carry):
            frame_stage(t, start)
            for i in range(planes):
                outgoing[side, pl.ds((i * tiles + t) * 2, 2), :] = first[i, t, pl.ds(8 if side == 0 else rows + 6, 2), :]
            return carry

        lax.fori_loop(0, tiles, body, 0)

        @pl.when(has_upper if side == 0 else has_lower)
        def _():
            row_copy(side).start()

    edge(0)
    edge(1)

    def take(t):
        arrive(t + 2)

        @pl.when(t + 2 + DEPTH < tiles + 2)
        def _():
            issue(t + 2 + DEPTH)

        def body(g, carry):
            frame_stage(t, pl.multiple_of(8 * g, 8))
            return carry

        lax.fori_loop(1, groups - 1, body, 0)

    def early(t, carry):
        take(t)
        return carry

    lax.fori_loop(0, LATE + 1, early, 0)

    for side in range(2):
        place = rows + 8 if side == 0 else 6
        there = has_lower if side == 0 else has_upper

        @pl.when(there)
        def _():
            row_copy(side).wait_recv()

            def body(t, carry):
                for i in range(planes):
                    first[i, t, pl.ds(place, 2), :] = incoming[side, pl.ds((i * tiles + t) * 2, 2), :]
                return carry

            lax.fori_loop(0, tiles, body, 0)

        @pl.when(jnp.logical_not(there))
        def _():
            def body(t, carry):
                for i in range(planes):
                    first[i, t, pl.ds(place, 2), :] = jnp.zeros((2, LANES), jnp.float32)
                return carry

            lax.fori_loop(0, tiles, body, 0)

    row_stage(0)

    def catch_up(t, carry):
        row_stage(t + 1)
        finish(t)
        return carry

    lax.fori_loop(0, LATE, catch_up, 0)

    def late(t, carry):
        take(t)
        row_stage(t)
        finish(t - 1)
        return carry

    lax.fori_loop(LATE + 1, tiles, late, 0)
    finish(tiles - 1)

    for side in range(2):

        @pl.when(has_upper if side == 0 else has_lower)
        def _():
            row_copy(side).wait_send()


def moments_kernel(boxes, weight, out, moments, parts, sem):
    depth, tiles, rows = weight.shape[0:3]
    slots = boxes.shape[1]

    def store(t):
        return pltpu.make_async_copy(weight.at[:, t], out.at[:, :, pl.ds(t * LANES, LANES)], sem.at[t])

    for t in range(tiles):
        store(t).start()
    frame_base = lax.axis_index("omega") * depth
    row_base = lax.axis_index("row") * rows
    sub = lax.broadcasted_iota(jnp.int32, (8, LANES), 0)
    lane = lax.broadcasted_iota(jnp.int32, (8, LANES), 1)
    half_f, half_r, half_c = ((BOX_F - 1) / 2.0, (BOX_R - 1) / 2.0, (BOX_C - 1) / 2.0)
    u_row = [((sub + 8 * j).astype(jnp.float32) - half_r) / half_r for j in range(2)]

    def box(b, carry):
        live = boxes[0, b] >= 0

        @pl.when(live)
        def _():
            f0 = boxes[0, b] - frame_base
            r0 = boxes[1, b] - row_base
            c0 = boxes[2, b]
            totals = None
            for side in range(2):
                tile = jnp.minimum(c0 // LANES + side, tiles - 1)
                distance = lane - (lax.rem(c0, LANES) - side * LANES)
                inside = (distance >= 0) & (distance < BOX_C)
                u_column = (distance.astype(jnp.float32) - half_c) / half_c
                plain = [None, None]
                framed = [None, None]
                for j in range(2):
                    for i in range(BOX_F):
                        w = weight[f0 + i, tile, pl.ds(r0 + 8 * j, 8), :]
                        m = w * ((i - half_f) / half_f)
                        plain[j] = w if i == 0 else plain[j] + w
                        framed[j] = m if i == 0 else framed[j] + m
                everything = plain[0] + plain[1]
                stats = [everything, framed[0] + framed[1], plain[0] * u_row[0] + plain[1] * u_row[1], everything * u_column]
                stats = [jnp.where(inside, s, 0.0) for s in stats]
                totals = stats if side == 0 else [p + q for p, q in zip(totals, stats)]
            for s in range(4):
                parts[s, pl.ds(pl.multiple_of(b * 8, 8), 8), :] = totals[s]

        @pl.when(jnp.logical_not(live))
        def _():
            for s in range(4):
                parts[s, pl.ds(pl.multiple_of(b * 8, 8), 8), :] = jnp.zeros((8, LANES), jnp.float32)

        return carry

    lax.fori_loop(0, slots, box, 0)
    ones = jnp.ones((8, LANES), jnp.float32)
    lines = []
    for s in range(4):
        total = parts[s, pl.ds(0, slots, stride=8), :]
        for j in range(1, 8):
            total = total + parts[s, pl.ds(j, slots, stride=8), :]
        sums = lax.dot_general(ones, total, (((1,), (1,)), ((), ())), precision=lax.Precision.HIGHEST, preferred_element_type=jnp.float32)
        lines.append(sums[0:1, :])
    moments[...] = jnp.concatenate(lines, axis=0) * (1.0 / (BOX_F * BOX_R * BOX_C))
    for t in range(tiles):
        store(t).wait()


def on_device(n_omega, n_row, frames, thresholds, spot_boxes):
    depth, rows, columns = frames.shape
    tiles = columns // LANES
    planes = depth + 2
    slots = spot_boxes.shape[1]
    vmem = functools.partial(pl.BlockSpec, memory_space=pltpu.VMEM)
    smem = functools.partial(pl.BlockSpec, memory_space=pltpu.SMEM)
    anywhere = functools.partial(pl.BlockSpec, memory_space=pl.ANY)
    weight = pl.pallas_call(
        functools.partial(spread_kernel, n_omega, n_row),
        out_shape=pltpu.VMEM((depth, tiles, rows, LANES), jnp.float32),
        in_specs=[pl.BlockSpec(memory_space=pltpu.HBM), pl.BlockSpec(memory_space=pltpu.HBM)],
        out_specs=vmem(),
        scratch_shapes=[
            pltpu.SMEM((rows,), jnp.int32),
            pltpu.VMEM((depth + 2 * REACH, tiles, rows, LANES), jnp.float32),
            pltpu.VMEM((planes, tiles, rows + 16, LANES), jnp.float32),
            pltpu.VMEM((planes, tiles + 2, rows + 8, LANES), jnp.float32),
            pltpu.VMEM((depth, rows + 8, LANES), jnp.float32),
            pltpu.VMEM((planes, rows + 8, LANES), jnp.float32),
            pltpu.VMEM((rows, LANES), jnp.float32),
            pltpu.VMEM((2, planes * tiles * 2, LANES), jnp.float32),
            pltpu.VMEM((2, planes * tiles * 2, LANES), jnp.float32),
            pltpu.SemaphoreType.DMA,
            pltpu.SemaphoreType.DMA((tiles,)),
            pltpu.SemaphoreType.DMA((2, tiles + 2)),
            pltpu.SemaphoreType.DMA((2, tiles + 2)),
            pltpu.SemaphoreType.DMA((2,)),
            pltpu.SemaphoreType.DMA((2,)),
        ],
        compiler_params=pltpu.CompilerParams(collective_id=0, has_side_effects=True, vmem_limit_bytes=54 << 20),
        name="spread",
    )(frames, thresholds)
    return pl.pallas_call(
        moments_kernel,
        out_shape=(jax.ShapeDtypeStruct(frames.shape, jnp.float32), jax.ShapeDtypeStruct((4, slots), jnp.float32)),
        in_specs=[smem(), vmem()],
        out_specs=(anywhere(), vmem()),
        scratch_shapes=[pltpu.VMEM((4, slots * 8, LANES), jnp.float32), pltpu.SemaphoreType.DMA((tiles,))],
        compiler_params=pltpu.CompilerParams(vmem_limit_bytes=8 << 20),
        name="moments",
    )(spot_boxes, weight)


def solution(mesh):
    return jax.shard_map(
        functools.partial(on_device, mesh.shape["omega"], mesh.shape["row"]),
        mesh=mesh,
        in_specs=(P("omega", "row", None), P("row"), P(None, ("omega", "row"))),
        out_specs=(P("omega", "row", None), P(None, ("omega", "row"))),
        check_vma=False,
    )
```

```python
import functools

import jax
import jax.numpy as jnp
from jax import lax
from jax.experimental import pallas as pl
from jax.experimental.pallas import tpu as pltpu
from jax.sharding import PartitionSpec as P

BW = 4
REACH = BW + 2
BOX_F = 8
BOX_R = 16
BOX_C = 16
SHARP = 8.0
LOG2E = 1.4426950408889634
BIG = 3.0e38
LANES = 128
DEPTH = 3
LATE = 1
BLOCK = 6
MESH = pl.DeviceIdType.MESH


def spread_kernel(n_omega, n_row, frames, limits, weight, thresholds, x, first, second, smooth, wide, level, mix, outgoing, incoming, limit_sem, load_sem, send_sem, recv_sem, row_send, row_recv):
    depth, rows = (frames.shape[0], frames.shape[1])
    tiles = frames.shape[2] // LANES
    groups = rows // 8
    planes = depth + 2
    tall = rows + 8
    omega, row = (lax.axis_index("omega"), lax.axis_index("row"))
    after, before = (lax.rem(omega + 1, n_omega), lax.rem(omega + n_omega - 1, n_omega))
    has_upper, has_lower = (row > 0, row < n_row - 1)

    def load(part, t):
        start, count = ((0, 8), (rows - 8, 8), (8, rows - 16))[part]
        return pltpu.make_async_copy(
            frames.at[:, pl.ds(start, count), pl.ds(t * LANES, LANES)], x.at[pl.ds(REACH, depth), t, pl.ds(start, count), :], load_sem.at[part, t]
        )

    limits_copy = pltpu.make_async_copy(limits, thresholds, limit_sem)
    for part in range(3):
        for t in range(tiles):
            load(part, t).start()
    limits_copy.start()

    barrier = pltpu.get_barrier_semaphore()
    for neighbour in (before, after):
        pl.semaphore_signal(barrier, inc=1, device_id=(neighbour, row), device_id_type=MESH)

    @pl.when(has_upper)
    def _():
        pl.semaphore_signal(barrier, inc=1, device_id=(omega, row - 1), device_id_type=MESH)

    @pl.when(has_lower)
    def _():
        pl.semaphore_signal(barrier, inc=1, device_id=(omega, row + 1), device_id_type=MESH)

    sub = lax.broadcasted_iota(jnp.int32, (8, LANES), 0)

    def prepare():
        limits_copy.wait()
        for g in range(groups):
            tile = jnp.full((8, LANES), thresholds[g * 8].astype(jnp.float32))
            for j in range(1, 8):
                tile = jnp.where(sub == j, thresholds[g * 8 + j].astype(jnp.float32), tile)
            level[g * 8 : g * 8 + 8, :] = tile
        blank = jnp.zeros((tall, LANES), jnp.float32)
        for i in range(planes):
            second[0, i * tall : (i + 1) * tall, :] = blank
            second[tiles + 1, i * tall : (i + 1) * tall, :] = blank
        last = LANES - 1
        size = (LANES, LANES)
        source, place = (lax.broadcasted_iota(jnp.int32, size, 0), lax.broadcasted_iota(jnp.int32, size, 1))

        def taps(pairs):
            total = jnp.zeros(size, jnp.float32)
            for test, value in pairs:
                total = total + jnp.where(test, value, 0.0)
            return total.astype(jnp.bfloat16)

        at_first, at_last = (place == 0, place == last)
        mix[0:LANES, 0:LANES] = taps([(source == place, 2.0), (source == place - 1, 1.0), (source == place + 1, 1.0)])
        mix[LANES:, 0:LANES] = taps([(at_first & (source == last), 1.0), (at_last & (source == 0), 1.0)])
        mix[0:LANES, LANES:] = taps([(at_first & (source == last), 1.0), (at_last & (source == 0), 1.0)])
        mix[LANES:, LANES:] = taps(
            [(at_first & (source == 0), 2.0), (at_first & (source == 1), 1.0), (at_last & (source == last), 2.0), (at_last & (source == last - 1), 1.0)]
        )

    def piece(start, chunk):
        planes_of = pl.ds(start, REACH)
        if isinstance(chunk, int) and chunk < 2:
            return x.at[planes_of, :, pl.ds(0 if chunk == 0 else rows - 8, 8), :]
        return x.at[planes_of, chunk - 2, pl.ds(8, rows - 16), :]

    def copies(chunk):
        to_before = pltpu.make_async_remote_copy(
            src_ref=piece(REACH, chunk), dst_ref=piece(REACH + depth, chunk), send_sem=send_sem.at[0, chunk], recv_sem=recv_sem.at[0, chunk], device_id=(before, row), device_id_type=MESH
        )
        to_after = pltpu.make_async_remote_copy(
            src_ref=piece(depth, chunk), dst_ref=piece(0, chunk), send_sem=send_sem.at[1, chunk], recv_sem=recv_sem.at[1, chunk], device_id=(after, row), device_id_type=MESH
        )
        return (to_before, to_after)

    def row_copy(side):
        return pltpu.make_async_remote_copy(
            src_ref=outgoing.at[side], dst_ref=incoming.at[side], send_sem=row_send.at[side], recv_sem=row_recv.at[side], device_id=(omega, row - 1 if side == 0 else row + 1), device_id_type=MESH
        )

    for t in range(tiles):
        load(0, t).wait()
    pl.semaphore_wait(barrier, 2 + has_upper.astype(jnp.int32) + has_lower.astype(jnp.int32))

    def issue(chunk):
        for copy in copies(chunk):
            copy.start()

    def arrive(chunk):
        for copy in copies(chunk):
            copy.wait_recv()
        for copy in copies(chunk):
            copy.wait_send()

    def frame_stage(t, start):
        v = [x[j, t, pl.ds(start, 8), :] for j in range(depth + 2 * REACH)]
        s2 = [v[j] + v[j + 1] for j in range(len(v) - 1)]
        s4 = [s2[j] + s2[j + 2] for j in range(len(s2) - 2)]
        s8 = [s4[j] + s4[j + 4] for j in range(len(s4) - 4)]
        c = [v[j + BW] - (s8[j] + v[j + 2 * BW]) * (1.0 / (2 * BW + 1)) for j in range(depth + 4)]
        p = [c[j] + c[j + 1] for j in range(depth + 3)]
        for i in range(planes):
            first[i, t, pl.ds(start + 8, 8), :] = p[i] + p[i + 1]

    def row_stage(t):
        def body(k, carry):
            for i in range(planes):
                up = first[i, t, pl.ds(8 * k + 6, 8), :]
                mid = first[i, t, pl.ds(8 * k + 7, 8), :]
                down = first[i, t, pl.ds(8 * k + 8, 8), :]
                second[t + 1, pl.ds(pl.multiple_of(i * tall + 8 * k, 8), 8), :] = (up + down) + (mid + mid)
            return carry

        lax.fori_loop(0, groups + 1, body, 0)

    def column_stage(t):
        size = (BLOCK * tall, LANES)
        lane = lax.broadcasted_iota(jnp.int32, size, 1)
        left_edge, right_edge = (lane == 0, lane == LANES - 1)
        left_half = lane >= LANES // 2
        low = jnp.where(t == 0, -BIG, BIG)
        high = jnp.where(t == tiles - 1, -BIG, BIG)
        bound = jnp.where(left_half, low, high)

        def body(m, carry):
            at = pl.ds(pl.multiple_of(m * (BLOCK * tall), 8), BLOCK * tall)
            middle = second[t + 1, at, :]
            whole = jnp.concatenate([middle, jnp.where(left_half, second[t, at, :], second[t + 2, at, :])], axis=1)
            upper = whole.astype(jnp.bfloat16)
            lower = (whole - upper.astype(jnp.float32)).astype(jnp.bfloat16)
            out = jnp.dot(upper, mix[...], preferred_element_type=jnp.float32) + jnp.dot(lower, mix[...], preferred_element_type=jnp.float32)
            value = out[:, 0:LANES]
            beside = jnp.minimum(out[:, LANES:], bound)
            from_left = pltpu.roll(jnp.where(right_edge, beside, value), 1, 1)
            from_right = pltpu.roll(jnp.where(left_edge, beside, value), LANES - 1, 1)
            wide[at, :] = jnp.maximum(jnp.maximum(from_left, from_right), value)
            smooth[at, :] = value
            return carry

        lax.fori_loop(0, planes // BLOCK, body, 0)

        @pl.when(jnp.logical_not(has_upper))
        def _():
            for i in range(planes):
                wide[i * tall : i * tall + 1, :] = jnp.full((1, LANES), -BIG)

        @pl.when(jnp.logical_not(has_lower))
        def _():
            for i in range(planes):
                wide[i * tall + rows + 1 : i * tall + rows + 2, :] = jnp.full((1, LANES), -BIG)

    def weight_stage(t):
        def body(g, carry):
            start = pl.multiple_of(8 * g, 8)
            limit = level[pl.ds(start, 8), :]
            columns = []
            for i in range(planes):
                up = wide[pl.ds(i * tall + 8 * g, 8), :]
                mid = wide[pl.ds(i * tall + 8 * g + 1, 8), :]
                down = wide[pl.ds(i * tall + 8 * g + 2, 8), :]
                columns.append(jnp.maximum(jnp.maximum(up, down), mid))
                if i >= 2:
                    highest = jnp.maximum(jnp.maximum(columns[i - 2], columns[i - 1]), columns[i])
                    value = smooth[pl.ds((i - 1) * tall + 8 * g + 1, 8), :]
                    sharp = jnp.exp2((value - highest) * (SHARP * LOG2E / 64.0))
                    weight[i - 2, t, pl.ds(start, 8), :] = sharp * (jnp.maximum(value - limit, 0.0) * (1.0 / 64.0))
            return carry

        lax.fori_loop(0, groups, body, 0)

    def finish(t):
        column_stage(t)
        weight_stage(t)

    issue(0)
    for t in range(tiles):
        load(1, t).wait()
    issue(1)
    for t in range(tiles):
        load(2, t).wait()
    for chunk in range(2, DEPTH):
        issue(chunk)

    prepare()

    def edge(side):
        arrive(side)
        issue(side + DEPTH)
        start = 0 if side == 0 else rows - 8

        def body(t, carry):
            frame_stage(t, start)
            for i in range(planes):
                outgoing[side, pl.ds((i * tiles + t) * 2, 2), :] = first[i, t, pl.ds(8 if side == 0 else rows + 6, 2), :]
            return carry

        lax.fori_loop(0, tiles, body, 0)

        @pl.when(has_upper if side == 0 else has_lower)
        def _():
            row_copy(side).start()

    edge(0)
    edge(1)

    def take(t):
        arrive(t + 2)

        @pl.when(t + 2 + DEPTH < tiles + 2)
        def _():
            issue(t + 2 + DEPTH)

        def body(g, carry):
            frame_stage(t, pl.multiple_of(8 * g, 8))
            return carry

        lax.fori_loop(1, groups - 1, body, 0)

    def early(t, carry):
        take(t)
        return carry

    lax.fori_loop(0, LATE + 1, early, 0)

    for side in range(2):
        place = rows + 8 if side == 0 else 6
        there = has_lower if side == 0 else has_upper

        @pl.when(there)
        def _():
            row_copy(side).wait_recv()

            def body(t, carry):
                for i in range(planes):
                    first[i, t, pl.ds(place, 2), :] = incoming[side, pl.ds((i * tiles + t) * 2, 2), :]
                return carry

            lax.fori_loop(0, tiles, body, 0)

        @pl.when(jnp.logical_not(there))
        def _():
            def body(t, carry):
                for i in range(planes):
                    first[i, t, pl.ds(place, 2), :] = jnp.zeros((2, LANES), jnp.float32)
                return carry

            lax.fori_loop(0, tiles, body, 0)

    row_stage(0)

    def catch_up(t, carry):
        row_stage(t + 1)
        finish(t)
        return carry

    lax.fori_loop(0, LATE, catch_up, 0)

    def late(t, carry):
        take(t)
        row_stage(t)
        finish(t - 1)
        return carry

    lax.fori_loop(LATE + 1, tiles, late, 0)
    finish(tiles - 1)

    for side in range(2):

        @pl.when(has_upper if side == 0 else has_lower)
        def _():
            row_copy(side).wait_send()


def moments_kernel(boxes, weight, out, moments, parts, sem):
    depth, tiles, rows = weight.shape[0:3]
    slots = boxes.shape[1]

    def store(t):
        return pltpu.make_async_copy(weight.at[:, t], out.at[:, :, pl.ds(t * LANES, LANES)], sem.at[t])

    for t in range(tiles):
        store(t).start()
    frame_base = lax.axis_index("omega") * depth
    row_base = lax.axis_index("row") * rows
    sub = lax.broadcasted_iota(jnp.int32, (8, LANES), 0)
    lane = lax.broadcasted_iota(jnp.int32, (8, LANES), 1)
    half_f, half_r, half_c = ((BOX_F - 1) / 2.0, (BOX_R - 1) / 2.0, (BOX_C - 1) / 2.0)
    u_row = [((sub + 8 * j).astype(jnp.float32) - half_r) / half_r for j in range(2)]

    def box(b, carry):
        live = boxes[0, b] >= 0

        @pl.when(live)
        def _():
            f0 = boxes[0, b] - frame_base
            r0 = boxes[1, b] - row_base
            c0 = boxes[2, b]
            totals = None
            for side in range(2):
                tile = jnp.minimum(c0 // LANES + side, tiles - 1)
                distance = lane - (lax.rem(c0, LANES) - side * LANES)
                inside = (distance >= 0) & (distance < BOX_C)
                u_column = (distance.astype(jnp.float32) - half_c) / half_c
                plain = [None, None]
                framed = [None, None]
                for j in range(2):
                    for i in range(BOX_F):
                        w = weight[f0 + i, tile, pl.ds(r0 + 8 * j, 8), :]
                        m = w * ((i - half_f) / half_f)
                        plain[j] = w if i == 0 else plain[j] + w
                        framed[j] = m if i == 0 else framed[j] + m
                everything = plain[0] + plain[1]
                stats = [everything, framed[0] + framed[1], plain[0] * u_row[0] + plain[1] * u_row[1], everything * u_column]
                stats = [jnp.where(inside, s, 0.0) for s in stats]
                totals = stats if side == 0 else [p + q for p, q in zip(totals, stats)]
            for s in range(4):
                parts[s, pl.ds(pl.multiple_of(b * 8, 8), 8), :] = totals[s]

        @pl.when(jnp.logical_not(live))
        def _():
            for s in range(4):
                parts[s, pl.ds(pl.multiple_of(b * 8, 8), 8), :] = jnp.zeros((8, LANES), jnp.float32)

        return carry

    lax.fori_loop(0, slots, box, 0)
    ones = jnp.ones((8, LANES), jnp.float32)
    lines = []
    for s in range(4):
        total = parts[s, pl.ds(0, slots, stride=8), :]
        for j in range(1, 8):
            total = total + parts[s, pl.ds(j, slots, stride=8), :]
        sums = lax.dot_general(ones, total, (((1,), (1,)), ((), ())), precision=lax.Precision.HIGHEST, preferred_element_type=jnp.float32)
        lines.append(sums[0:1, :])
    moments[...] = jnp.concatenate(lines, axis=0) * (1.0 / (BOX_F * BOX_R * BOX_C))
    for t in range(tiles):
        store(t).wait()


def on_device(n_omega, n_row, frames, thresholds, spot_boxes):
    depth, rows, columns = frames.shape
    tiles = columns // LANES
    planes = depth + 2
    slots = spot_boxes.shape[1]
    vmem = functools.partial(pl.BlockSpec, memory_space=pltpu.VMEM)
    smem = functools.partial(pl.BlockSpec, memory_space=pltpu.SMEM)
    anywhere = functools.partial(pl.BlockSpec, memory_space=pl.ANY)
    weight = pl.pallas_call(
        functools.partial(spread_kernel, n_omega, n_row),
        out_shape=pltpu.VMEM((depth, tiles, rows, LANES), jnp.float32),
        in_specs=[pl.BlockSpec(memory_space=pltpu.HBM), pl.BlockSpec(memory_space=pltpu.HBM)],
        out_specs=vmem(),
        scratch_shapes=[
            pltpu.SMEM((rows,), jnp.int32),
            pltpu.VMEM((depth + 2 * REACH, tiles, rows, LANES), jnp.float32),
            pltpu.VMEM((planes, tiles, rows + 16, LANES), jnp.float32),
            pltpu.VMEM((tiles + 2, planes * (rows + 8), LANES), jnp.float32),
            pltpu.VMEM((planes * (rows + 8), LANES), jnp.float32),
            pltpu.VMEM((planes * (rows + 8), LANES), jnp.float32),
            pltpu.VMEM((rows, LANES), jnp.float32),
            pltpu.VMEM((2 * LANES, 2 * LANES), jnp.bfloat16),
            pltpu.VMEM((2, planes * tiles * 2, LANES), jnp.float32),
            pltpu.VMEM((2, planes * tiles * 2, LANES), jnp.float32),
            pltpu.SemaphoreType.DMA,
            pltpu.SemaphoreType.DMA((3, tiles)),
            pltpu.SemaphoreType.DMA((2, tiles + 2)),
            pltpu.SemaphoreType.DMA((2, tiles + 2)),
            pltpu.SemaphoreType.DMA((2,)),
            pltpu.SemaphoreType.DMA((2,)),
        ],
        compiler_params=pltpu.CompilerParams(collective_id=0, has_side_effects=True, vmem_limit_bytes=54 << 20),
        name="spread",
    )(frames, thresholds)
    return pl.pallas_call(
        moments_kernel,
        out_shape=(jax.ShapeDtypeStruct(frames.shape, jnp.float32), jax.ShapeDtypeStruct((4, slots), jnp.float32)),
        in_specs=[smem(), vmem()],
        out_specs=(anywhere(), vmem()),
        scratch_shapes=[pltpu.VMEM((4, slots * 8, LANES), jnp.float32), pltpu.SemaphoreType.DMA((tiles,))],
        compiler_params=pltpu.CompilerParams(vmem_limit_bytes=8 << 20),
        name="moments",
    )(spot_boxes, weight)


def solution(mesh):
    return jax.shard_map(
        functools.partial(on_device, mesh.shape["omega"], mesh.shape["row"]),
        mesh=mesh,
        in_specs=(P("omega", "row", None), P("row"), P(None, ("omega", "row"))),
        out_specs=(P("omega", "row", None), P(None, ("omega", "row"))),
        check_vma=False,
    )
```

```python
import functools

import jax
import jax.numpy as jnp
from jax import lax
from jax.experimental import pallas as pl
from jax.experimental.pallas import tpu as pltpu
from jax.sharding import PartitionSpec as P

BW = 4
REACH = BW + 2
BOX_F = 8
BOX_R = 16
BOX_C = 16
SHARP = 8.0
LOG2E = 1.4426950408889634
BIG = 3.0e38
LANES = 128
NEAR, FAR = (3, 1)
LATE = 1
BLOCK = 18
MESH = pl.DeviceIdType.MESH


def stages(n_row, first, second, smooth, wide, level, mix, weight):
    planes, tiles = (first.shape[0], first.shape[1])
    rows = level.shape[0]
    groups = rows // 8
    tall = rows + 8
    row = lax.axis_index("row")
    has_upper, has_lower = (row > 0, row < n_row - 1)

    def row_stage(t):
        def body(k, carry):
            for i in range(planes):
                up = first[i, t, pl.ds(8 * k + 6, 8), :]
                mid = first[i, t, pl.ds(8 * k + 7, 8), :]
                down = first[i, t, pl.ds(8 * k + 8, 8), :]
                second[t + 1, pl.ds(pl.multiple_of(i * tall + 8 * k, 8), 8), :] = (up + down) + (mid + mid)
            return carry

        lax.fori_loop(0, groups + 1, body, 0)

    def column_stage(t):
        size = (BLOCK * tall, LANES)
        lane = lax.broadcasted_iota(jnp.int32, size, 1)
        left_edge, right_edge = (lane == 0, lane == LANES - 1)
        left_half = lane >= LANES // 2
        low = jnp.where(t == 0, -BIG, BIG)
        high = jnp.where(t == tiles - 1, -BIG, BIG)
        bound = jnp.where(left_half, low, high)

        def body(m, carry):
            at = pl.ds(pl.multiple_of(m * (BLOCK * tall), 8), BLOCK * tall)
            middle = second[t + 1, at, :]
            whole = jnp.concatenate([middle, jnp.where(left_half, second[t, at, :], second[t + 2, at, :])], axis=1)
            upper = whole.astype(jnp.bfloat16)
            lower = (whole - upper.astype(jnp.float32)).astype(jnp.bfloat16)
            out = jnp.dot(upper, mix[...], preferred_element_type=jnp.float32) + jnp.dot(lower, mix[...], preferred_element_type=jnp.float32)
            value = out[:, 0:LANES]
            beside = jnp.minimum(out[:, LANES:], bound)
            from_left = pltpu.roll(jnp.where(right_edge, beside, value), 1, 1)
            from_right = pltpu.roll(jnp.where(left_edge, beside, value), LANES - 1, 1)
            wide[at, :] = jnp.maximum(jnp.maximum(from_left, from_right), value)
            smooth[at, :] = value
            return carry

        lax.fori_loop(0, planes // BLOCK, body, 0)

        @pl.when(jnp.logical_not(has_upper))
        def _():
            for i in range(planes):
                wide[i * tall : i * tall + 1, :] = jnp.full((1, LANES), -BIG)

        @pl.when(jnp.logical_not(has_lower))
        def _():
            for i in range(planes):
                wide[i * tall + rows + 1 : i * tall + rows + 2, :] = jnp.full((1, LANES), -BIG)

    def weight_stage(t):
        def body(g, carry):
            start = pl.multiple_of(8 * g, 8)
            limit = level[pl.ds(start, 8), :]
            columns = []
            for i in range(planes):
                up = wide[pl.ds(i * tall + 8 * g, 8), :]
                mid = wide[pl.ds(i * tall + 8 * g + 1, 8), :]
                down = wide[pl.ds(i * tall + 8 * g + 2, 8), :]
                columns.append(jnp.maximum(jnp.maximum(up, down), mid))
                if i >= 2:
                    highest = jnp.maximum(jnp.maximum(columns[i - 2], columns[i - 1]), columns[i])
                    value = smooth[pl.ds((i - 1) * tall + 8 * g + 1, 8), :]
                    sharp = jnp.exp2((value - highest) * (SHARP * LOG2E / 64.0))
                    weight[i - 2, t, pl.ds(start, 8), :] = sharp * (jnp.maximum(value - limit, 0.0) * (1.0 / 64.0))
            return carry

        lax.fori_loop(0, groups, body, 0)

    def finish(t):
        column_stage(t)
        weight_stage(t)

    return (row_stage, finish)


def spread_kernel(n_omega, n_row, frames, limits, weight, first, second, level, mix, thresholds, x, smooth, wide, outgoing, incoming, limit_sem, load_sem, send_sem, recv_sem, row_send, row_recv):
    depth, rows = (frames.shape[0], frames.shape[1])
    tiles = frames.shape[2] // LANES
    groups = rows // 8
    planes = depth + 2
    tall = rows + 8
    omega, row = (lax.axis_index("omega"), lax.axis_index("row"))
    after, before = (lax.rem(omega + 1, n_omega), lax.rem(omega + n_omega - 1, n_omega))
    has_upper, has_lower = (row > 0, row < n_row - 1)

    def load(part, t):
        start, count = ((0, 8), (rows - 8, 8), (8, rows - 16))[part]
        return pltpu.make_async_copy(
            frames.at[:, pl.ds(start, count), pl.ds(t * LANES, LANES)], x.at[pl.ds(REACH, depth), t, pl.ds(start, count), :], load_sem.at[part, t]
        )

    limits_copy = pltpu.make_async_copy(limits, thresholds, limit_sem)
    for part in range(3):
        for t in range(tiles):
            load(part, t).start()
    limits_copy.start()

    barrier = pltpu.get_barrier_semaphore()
    for neighbour in (before, after):
        pl.semaphore_signal(barrier, inc=1, device_id=(neighbour, row), device_id_type=MESH)

    @pl.when(has_upper)
    def _():
        pl.semaphore_signal(barrier, inc=1, device_id=(omega, row - 1), device_id_type=MESH)

    @pl.when(has_lower)
    def _():
        pl.semaphore_signal(barrier, inc=1, device_id=(omega, row + 1), device_id_type=MESH)

    sub = lax.broadcasted_iota(jnp.int32, (8, LANES), 0)

    def prepare():
        limits_copy.wait()
        for g in range(groups):
            tile = jnp.full((8, LANES), thresholds[g * 8].astype(jnp.float32))
            for j in range(1, 8):
                tile = jnp.where(sub == j, thresholds[g * 8 + j].astype(jnp.float32), tile)
            level[g * 8 : g * 8 + 8, :] = tile
        blank = jnp.zeros((tall, LANES), jnp.float32)
        for i in range(planes):
            second[0, i * tall : (i + 1) * tall, :] = blank
            second[tiles + 1, i * tall : (i + 1) * tall, :] = blank
        last = LANES - 1
        size = (LANES, LANES)
        source, place = (lax.broadcasted_iota(jnp.int32, size, 0), lax.broadcasted_iota(jnp.int32, size, 1))

        def taps(pairs):
            total = jnp.zeros(size, jnp.float32)
            for test, value in pairs:
                total = total + jnp.where(test, value, 0.0)
            return total.astype(jnp.bfloat16)

        at_first, at_last = (place == 0, place == last)
        mix[0:LANES, 0:LANES] = taps([(source == place, 2.0), (source == place - 1, 1.0), (source == place + 1, 1.0)])
        mix[LANES:, 0:LANES] = taps([(at_first & (source == last), 1.0), (at_last & (source == 0), 1.0)])
        mix[0:LANES, LANES:] = taps([(at_first & (source == last), 1.0), (at_last & (source == 0), 1.0)])
        mix[LANES:, LANES:] = taps(
            [(at_first & (source == 0), 2.0), (at_first & (source == 1), 1.0), (at_last & (source == last), 2.0), (at_last & (source == last - 1), 1.0)]
        )

    def piece(start, chunk):
        planes_of = pl.ds(start, REACH)
        if isinstance(chunk, int) and chunk < 2:
            return x.at[planes_of, :, pl.ds(0 if chunk == 0 else rows - 8, 8), :]
        return x.at[planes_of, chunk - 2, pl.ds(8, rows - 16), :]

    def copies(chunk):
        to_before = pltpu.make_async_remote_copy(
            src_ref=piece(REACH, chunk), dst_ref=piece(REACH + depth, chunk), send_sem=send_sem.at[0, chunk], recv_sem=recv_sem.at[0, chunk], device_id=(before, row), device_id_type=MESH
        )
        to_after = pltpu.make_async_remote_copy(
            src_ref=piece(depth, chunk), dst_ref=piece(0, chunk), send_sem=send_sem.at[1, chunk], recv_sem=recv_sem.at[1, chunk], device_id=(after, row), device_id_type=MESH
        )
        return (to_before, to_after)

    def row_copy(side):
        return pltpu.make_async_remote_copy(
            src_ref=outgoing.at[side], dst_ref=incoming.at[side], send_sem=row_send.at[side], recv_sem=row_recv.at[side], device_id=(omega, row - 1 if side == 0 else row + 1), device_id_type=MESH
        )

    for t in range(tiles):
        load(0, t).wait()
    pl.semaphore_wait(barrier, 2 + has_upper.astype(jnp.int32) + has_lower.astype(jnp.int32))

    def issue(chunk):
        for copy in copies(chunk):
            copy.start()

    corner = lax.rem(omega, 4)
    ahead = jnp.where((corner == 0) | (corner == 3), FAR, NEAR)

    def sent(chunk):
        for copy in copies(chunk):
            copy.wait_send()

    def arrive(chunk):
        for copy in copies(chunk):
            copy.wait_recv()

    def frame_stage(t, start):
        v = [x[j, t, pl.ds(start, 8), :] for j in range(depth + 2 * REACH)]
        s2 = [v[j] + v[j + 1] for j in range(len(v) - 1)]
        s4 = [s2[j] + s2[j + 2] for j in range(len(s2) - 2)]
        s8 = [s4[j] + s4[j + 4] for j in range(len(s4) - 4)]
        c = [v[j + BW] - (s8[j] + v[j + 2 * BW]) * (1.0 / (2 * BW + 1)) for j in range(depth + 4)]
        p = [c[j] + c[j + 1] for j in range(depth + 3)]
        for i in range(planes):
            first[i, t, pl.ds(start + 8, 8), :] = p[i] + p[i + 1]

    row_stage, finish = stages(n_row, first, second, smooth, wide, level, mix, weight)

    issue(0)
    for t in range(tiles):
        load(1, t).wait()

    @pl.when(ahead >= 2)
    def _():
        issue(1)

    for t in range(tiles):
        load(2, t).wait()
    for chunk in range(2, max(NEAR, FAR)):

        @pl.when(ahead > chunk)
        def _():
            issue(chunk)

    prepare()

    def edge(side):
        sent(side)
        if side == 0 and min(NEAR, FAR) == 1:

            @pl.when(ahead == 1)
            def _():
                issue(1)

            @pl.when(ahead > 1)
            def _():
                issue(ahead)

        else:
            issue(ahead + side)
        arrive(side)
        start = 0 if side == 0 else rows - 8

        def body(t, carry):
            frame_stage(t, start)
            for i in range(planes):
                outgoing[side, pl.ds((i * tiles + t) * 2, 2), :] = first[i, t, pl.ds(8 if side == 0 else rows + 6, 2), :]
            return carry

        lax.fori_loop(0, tiles, body, 0)

        @pl.when(has_upper if side == 0 else has_lower)
        def _():
            row_copy(side).start()

    edge(0)
    edge(1)

    def take(t):
        sent(t + 2)

        @pl.when(t + 2 + ahead < tiles + 2)
        def _():
            issue(t + 2 + ahead)

        arrive(t + 2)

        def body(g, carry):
            frame_stage(t, pl.multiple_of(8 * g, 8))
            return carry

        lax.fori_loop(1, groups - 1, body, 0)

    def early(t, carry):
        take(t)
        return carry

    lax.fori_loop(0, LATE + 1, early, 0)

    for side in range(2):
        place = rows + 8 if side == 0 else 6
        there = has_lower if side == 0 else has_upper

        @pl.when(there)
        def _():
            row_copy(side).wait_recv()

            def body(t, carry):
                for i in range(planes):
                    first[i, t, pl.ds(place, 2), :] = incoming[side, pl.ds((i * tiles + t) * 2, 2), :]
                return carry

            lax.fori_loop(0, tiles, body, 0)

        @pl.when(jnp.logical_not(there))
        def _():
            def body(t, carry):
                for i in range(planes):
                    first[i, t, pl.ds(place, 2), :] = jnp.zeros((2, LANES), jnp.float32)
                return carry

            lax.fori_loop(0, tiles, body, 0)

    row_stage(0)

    def catch_up(t, carry):
        row_stage(t + 1)
        finish(t)
        return carry

    lax.fori_loop(0, LATE, catch_up, 0)

    def late(t, carry):
        take(t)
        row_stage(t)
        finish(t - 1)
        return carry

    lax.fori_loop(LATE + 1, tiles - 1, late, 0)
    take(tiles - 1)

    for side in range(2):

        @pl.when(has_upper if side == 0 else has_lower)
        def _():
            row_copy(side).wait_send()


def moments_kernel(n_row, boxes, first, second_in, level, mix, weight_in, out, moments, second, weight, smooth, wide, parts, sem):
    depth, tiles, rows = weight.shape[0:3]
    slots = boxes.shape[1]

    def store(t):
        return pltpu.make_async_copy(weight.at[:, t], out.at[:, :, pl.ds(t * LANES, LANES)], sem.at[t])

    for t in range(tiles - 2):
        store(t).start()
    row_stage, finish = stages(n_row, first, second, smooth, wide, level, mix, weight)
    row_stage(tiles - 1)

    def tail(t, carry):
        finish(t)
        store(t).start()
        return carry

    lax.fori_loop(tiles - 2, tiles, tail, 0)
    frame_base = lax.axis_index("omega") * depth
    row_base = lax.axis_index("row") * rows
    sub = lax.broadcasted_iota(jnp.int32, (8, LANES), 0)
    lane = lax.broadcasted_iota(jnp.int32, (8, LANES), 1)
    half_f, half_r, half_c = ((BOX_F - 1) / 2.0, (BOX_R - 1) / 2.0, (BOX_C - 1) / 2.0)
    u_row = [((sub + 8 * j).astype(jnp.float32) - half_r) / half_r for j in range(2)]

    def box(b, carry):
        live = boxes[0, b] >= 0

        @pl.when(live)
        def _():
            f0 = boxes[0, b] - frame_base
            r0 = boxes[1, b] - row_base
            c0 = boxes[2, b]
            totals = None
            for side in range(2):
                tile = jnp.minimum(c0 // LANES + side, tiles - 1)
                distance = lane - (lax.rem(c0, LANES) - side * LANES)
                inside = (distance >= 0) & (distance < BOX_C)
                u_column = (distance.astype(jnp.float32) - half_c) / half_c
                plain = [None, None]
                framed = [None, None]
                for j in range(2):
                    for i in range(BOX_F):
                        w = weight[f0 + i, tile, pl.ds(r0 + 8 * j, 8), :]
                        m = w * ((i - half_f) / half_f)
                        plain[j] = w if i == 0 else plain[j] + w
                        framed[j] = m if i == 0 else framed[j] + m
                everything = plain[0] + plain[1]
                stats = [everything, framed[0] + framed[1], plain[0] * u_row[0] + plain[1] * u_row[1], everything * u_column]
                stats = [jnp.where(inside, s, 0.0) for s in stats]
                totals = stats if side == 0 else [p + q for p, q in zip(totals, stats)]
            for s in range(4):
                parts[s, pl.ds(pl.multiple_of(b * 8, 8), 8), :] = totals[s]

        @pl.when(jnp.logical_not(live))
        def _():
            for s in range(4):
                parts[s, pl.ds(pl.multiple_of(b * 8, 8), 8), :] = jnp.zeros((8, LANES), jnp.float32)

        return carry

    lax.fori_loop(0, slots, box, 0)
    ones = jnp.ones((8, LANES), jnp.float32)
    lines = []
    for s in range(4):
        total = parts[s, pl.ds(0, slots, stride=8), :]
        for j in range(1, 8):
            total = total + parts[s, pl.ds(j, slots, stride=8), :]
        sums = lax.dot_general(ones, total, (((1,), (1,)), ((), ())), precision=lax.Precision.HIGHEST, preferred_element_type=jnp.float32)
        lines.append(sums[0:1, :])
    moments[...] = jnp.concatenate(lines, axis=0) * (1.0 / (BOX_F * BOX_R * BOX_C))
    for t in range(tiles):
        store(t).wait()


def on_device(n_omega, n_row, frames, thresholds, spot_boxes):
    depth, rows, columns = frames.shape
    tiles = columns // LANES
    planes = depth + 2
    slots = spot_boxes.shape[1]
    vmem = functools.partial(pl.BlockSpec, memory_space=pltpu.VMEM)
    smem = functools.partial(pl.BlockSpec, memory_space=pltpu.SMEM)
    anywhere = functools.partial(pl.BlockSpec, memory_space=pl.ANY)
    tall = planes * (rows + 8)
    kept = (
        pltpu.VMEM((depth, tiles, rows, LANES), jnp.float32),
        pltpu.VMEM((planes, tiles, rows + 16, LANES), jnp.float32),
        pltpu.VMEM((tiles + 2, tall, LANES), jnp.float32),
        pltpu.VMEM((rows, LANES), jnp.float32),
        pltpu.VMEM((2 * LANES, 2 * LANES), jnp.bfloat16),
    )
    weight, first, second, level, mix = pl.pallas_call(
        functools.partial(spread_kernel, n_omega, n_row),
        out_shape=kept,
        in_specs=[pl.BlockSpec(memory_space=pltpu.HBM), pl.BlockSpec(memory_space=pltpu.HBM)],
        out_specs=tuple(vmem() for _ in kept),
        scratch_shapes=[
            pltpu.SMEM((rows,), jnp.int32),
            pltpu.VMEM((depth + 2 * REACH, tiles, rows, LANES), jnp.float32),
            pltpu.VMEM((tall, LANES), jnp.float32),
            pltpu.VMEM((tall, LANES), jnp.float32),
            pltpu.VMEM((2, planes * tiles * 2, LANES), jnp.float32),
            pltpu.VMEM((2, planes * tiles * 2, LANES), jnp.float32),
            pltpu.SemaphoreType.DMA,
            pltpu.SemaphoreType.DMA((3, tiles)),
            pltpu.SemaphoreType.DMA((2, tiles + 2)),
            pltpu.SemaphoreType.DMA((2, tiles + 2)),
            pltpu.SemaphoreType.DMA((2,)),
            pltpu.SemaphoreType.DMA((2,)),
        ],
        compiler_params=pltpu.CompilerParams(collective_id=0, has_side_effects=True, vmem_limit_bytes=40 << 20),
        name="spread",
    )(frames, thresholds)
    out = pl.pallas_call(
        functools.partial(moments_kernel, n_row),
        out_shape=(jax.ShapeDtypeStruct(frames.shape, jnp.float32), jax.ShapeDtypeStruct((4, slots), jnp.float32), kept[2], kept[0]),
        in_specs=[smem(), vmem(), vmem(), vmem(), vmem(), vmem()],
        out_specs=(anywhere(), vmem(), vmem(), vmem()),
        scratch_shapes=[
            pltpu.VMEM((tall, LANES), jnp.float32),
            pltpu.VMEM((tall, LANES), jnp.float32),
            pltpu.VMEM((4, slots * 8, LANES), jnp.float32),
            pltpu.SemaphoreType.DMA((tiles,)),
        ],
        input_output_aliases={2: 2, 5: 3},
        compiler_params=pltpu.CompilerParams(vmem_limit_bytes=8 << 20),
        name="moments",
    )(spot_boxes, first, second, level, mix, weight)
    return out[0:2]


def solution(mesh):
    return jax.shard_map(
        functools.partial(on_device, mesh.shape["omega"], mesh.shape["row"]),
        mesh=mesh,
        in_specs=(P("omega", "row", None), P("row"), P(None, ("omega", "row"))),
        out_specs=(P("omega", "row", None), P(None, ("omega", "row"))),
        check_vma=False,
    )
```

```python
import functools

import jax
import jax.numpy as jnp
from jax import lax
from jax.experimental import pallas as pl
from jax.experimental.pallas import tpu as pltpu
from jax.sharding import PartitionSpec as P

BW = 4
REACH = BW + 2
BOX_F = 8
BOX_R = 16
BOX_C = 16
SHARP = 8.0
LOG2E = 1.4426950408889634
BIG = 3.0e38
LANES = 128
NEAR, FAR = (3, 1)
LATE = 1
BLOCK = 18
ROW_STEP = 3
MESH = pl.DeviceIdType.MESH


def stages(n_row, first, second, smooth, wide, level, mix, weight):
    planes, tiles = (first.shape[0], first.shape[1])
    rows = level.shape[0]
    groups = rows // 8
    tall = rows + 8
    row = lax.axis_index("row")
    has_upper, has_lower = (row > 0, row < n_row - 1)

    def row_stage(t):
        def body(step, carry):
            for j in range(ROW_STEP):
                k = step * ROW_STEP + j
                for i in range(planes):
                    up = first[i, t, pl.ds(8 * k + 6, 8), :]
                    mid = first[i, t, pl.ds(8 * k + 7, 8), :]
                    down = first[i, t, pl.ds(8 * k + 8, 8), :]
                    second[t + 1, pl.ds(pl.multiple_of(i * tall + 8 * k, 8), 8), :] = (up + down) + (mid + mid)
            return carry

        lax.fori_loop(0, (groups + 1) // ROW_STEP, body, 0)

    def column_stage(t):
        size = (BLOCK * tall, LANES)
        lane = lax.broadcasted_iota(jnp.int32, size, 1)
        left_edge, right_edge = (lane == 0, lane == LANES - 1)
        left_half = lane >= LANES // 2
        low = jnp.where(t == 0, -BIG, BIG)
        high = jnp.where(t == tiles - 1, -BIG, BIG)
        bound = jnp.where(left_half, low, high)

        def body(m, carry):
            at = pl.ds(pl.multiple_of(m * (BLOCK * tall), 8), BLOCK * tall)
            middle = second[t + 1, at, :]
            whole = jnp.concatenate([middle, jnp.where(left_half, second[t, at, :], second[t + 2, at, :])], axis=1)
            upper = whole.astype(jnp.bfloat16)
            lower = (whole - upper.astype(jnp.float32)).astype(jnp.bfloat16)
            out = jnp.dot(upper, mix[...], preferred_element_type=jnp.float32) + jnp.dot(lower, mix[...], preferred_element_type=jnp.float32)
            value = out[:, 0:LANES]
            beside = jnp.minimum(out[:, LANES:], bound)
            from_left = pltpu.roll(jnp.where(right_edge, beside, value), 1, 1)
            from_right = pltpu.roll(jnp.where(left_edge, beside, value), LANES - 1, 1)
            wide[at, :] = jnp.maximum(jnp.maximum(from_left, from_right), value)
            smooth[at, :] = value
            return carry

        lax.fori_loop(0, planes // BLOCK, body, 0)

        @pl.when(jnp.logical_not(has_upper))
        def _():
            for i in range(planes):
                wide[i * tall : i * tall + 1, :] = jnp.full((1, LANES), -BIG)

        @pl.when(jnp.logical_not(has_lower))
        def _():
            for i in range(planes):
                wide[i * tall + rows + 1 : i * tall + rows + 2, :] = jnp.full((1, LANES), -BIG)

    def weight_stage(t):
        def group(g):
            start = pl.multiple_of(8 * g, 8)
            limit = level[pl.ds(start, 8), :]
            columns = []
            for i in range(planes):
                up = wide[pl.ds(i * tall + 8 * g, 8), :]
                mid = wide[pl.ds(i * tall + 8 * g + 1, 8), :]
                down = wide[pl.ds(i * tall + 8 * g + 2, 8), :]
                columns.append(jnp.maximum(jnp.maximum(up, down), mid))
                if i >= 2:
                    highest = jnp.maximum(jnp.maximum(columns[i - 2], columns[i - 1]), columns[i])
                    value = smooth[pl.ds((i - 1) * tall + 8 * g + 1, 8), :]
                    sharp = jnp.exp2((value - highest) * (SHARP * LOG2E / 64.0))
                    weight[i - 2, t, pl.ds(start, 8), :] = sharp * (jnp.maximum(value - limit, 0.0) * (1.0 / 64.0))

        def body(step, carry):
            for j in range(2):
                group(step * 2 + j)
            return carry

        lax.fori_loop(0, groups // 2, body, 0)

    def finish(t):
        column_stage(t)
        weight_stage(t)

    return (row_stage, finish)


def spread_kernel(n_omega, n_row, frames, limits, weight, first, second, level, mix, thresholds, x, smooth, wide, outgoing, incoming, limit_sem, load_sem, send_sem, recv_sem, row_send, row_recv):
    depth, rows = (frames.shape[0], frames.shape[1])
    tiles = frames.shape[2] // LANES
    groups = rows // 8
    planes = depth + 2
    tall = rows + 8
    omega, row = (lax.axis_index("omega"), lax.axis_index("row"))
    after, before = (lax.rem(omega + 1, n_omega), lax.rem(omega + n_omega - 1, n_omega))
    has_upper, has_lower = (row > 0, row < n_row - 1)

    def load(part, t):
        start, count = ((0, 8), (rows - 8, 8), (8, rows - 16))[part]
        return pltpu.make_async_copy(
            frames.at[:, pl.ds(start, count), pl.ds(t * LANES, LANES)], x.at[pl.ds(REACH, depth), t, pl.ds(start, count), :], load_sem.at[part, t]
        )

    barrier = pltpu.get_barrier_semaphore()
    for neighbour in (before, after):
        pl.semaphore_signal(barrier, inc=1, device_id=(neighbour, row), device_id_type=MESH)

    @pl.when(has_upper)
    def _():
        pl.semaphore_signal(barrier, inc=1, device_id=(omega, row - 1), device_id_type=MESH)

    @pl.when(has_lower)
    def _():
        pl.semaphore_signal(barrier, inc=1, device_id=(omega, row + 1), device_id_type=MESH)

    limits_copy = pltpu.make_async_copy(limits, thresholds, limit_sem)
    for part in range(3):
        for t in range(tiles):
            load(part, t).start()
    limits_copy.start()

    sub = lax.broadcasted_iota(jnp.int32, (8, LANES), 0)

    def prepare():
        limits_copy.wait()
        for g in range(groups):
            tile = jnp.full((8, LANES), thresholds[g * 8].astype(jnp.float32))
            for j in range(1, 8):
                tile = jnp.where(sub == j, thresholds[g * 8 + j].astype(jnp.float32), tile)
            level[g * 8 : g * 8 + 8, :] = tile
        blank = jnp.zeros((tall, LANES), jnp.float32)
        for i in range(planes):
            second[0, i * tall : (i + 1) * tall, :] = blank
            second[tiles + 1, i * tall : (i + 1) * tall, :] = blank
        last = LANES - 1
        size = (LANES, LANES)
        source, place = (lax.broadcasted_iota(jnp.int32, size, 0), lax.broadcasted_iota(jnp.int32, size, 1))

        def taps(pairs):
            total = jnp.zeros(size, jnp.float32)
            for test, value in pairs:
                total = total + jnp.where(test, value, 0.0)
            return total.astype(jnp.bfloat16)

        at_first, at_last = (place == 0, place == last)
        mix[0:LANES, 0:LANES] = taps([(source == place, 2.0), (source == place - 1, 1.0), (source == place + 1, 1.0)])
        mix[LANES:, 0:LANES] = taps([(at_first & (source == last), 1.0), (at_last & (source == 0), 1.0)])
        mix[0:LANES, LANES:] = taps([(at_first & (source == last), 1.0), (at_last & (source == 0), 1.0)])
        mix[LANES:, LANES:] = taps(
            [(at_first & (source == 0), 2.0), (at_first & (source == 1), 1.0), (at_last & (source == last), 2.0), (at_last & (source == last - 1), 1.0)]
        )

    def piece(start, chunk):
        planes_of = pl.ds(start, REACH)
        if isinstance(chunk, int) and chunk < 2:
            return x.at[planes_of, :, pl.ds(0 if chunk == 0 else rows - 8, 8), :]
        return x.at[planes_of, chunk - 2, pl.ds(8, rows - 16), :]

    def copies(chunk):
        to_before = pltpu.make_async_remote_copy(
            src_ref=piece(REACH, chunk), dst_ref=piece(REACH + depth, chunk), send_sem=send_sem.at[0, chunk], recv_sem=recv_sem.at[0, chunk], device_id=(before, row), device_id_type=MESH
        )
        to_after = pltpu.make_async_remote_copy(
            src_ref=piece(depth, chunk), dst_ref=piece(0, chunk), send_sem=send_sem.at[1, chunk], recv_sem=recv_sem.at[1, chunk], device_id=(after, row), device_id_type=MESH
        )
        return (to_before, to_after)

    def row_copy(side):
        return pltpu.make_async_remote_copy(
            src_ref=outgoing.at[side], dst_ref=incoming.at[side], send_sem=row_send.at[side], recv_sem=row_recv.at[side], device_id=(omega, row - 1 if side == 0 else row + 1), device_id_type=MESH
        )

    for t in range(tiles):
        load(0, t).wait()
    pl.semaphore_wait(barrier, 2 + has_upper.astype(jnp.int32) + has_lower.astype(jnp.int32))

    def issue(chunk):
        for copy in copies(chunk):
            copy.start()

    corner = lax.rem(omega, 4)
    ahead = jnp.where((corner == 0) | (corner == 3), FAR, NEAR)

    def sent(chunk):
        for copy in copies(chunk):
            copy.wait_send()

    def arrive(chunk):
        for copy in copies(chunk):
            copy.wait_recv()

    def frame_stage(t, start):
        v = [x[j, t, pl.ds(start, 8), :] for j in range(depth + 2 * REACH)]
        s2 = [v[j] + v[j + 1] for j in range(len(v) - 1)]
        s4 = [s2[j] + s2[j + 2] for j in range(len(s2) - 2)]
        s8 = [s4[j] + s4[j + 4] for j in range(len(s4) - 4)]
        c = [v[j + BW] - (s8[j] + v[j + 2 * BW]) * (1.0 / (2 * BW + 1)) for j in range(depth + 4)]
        p = [c[j] + c[j + 1] for j in range(depth + 3)]
        for i in range(planes):
            first[i, t, pl.ds(start + 8, 8), :] = p[i] + p[i + 1]

    row_stage, finish = stages(n_row, first, second, smooth, wide, level, mix, weight)

    issue(0)
    for t in range(tiles):
        load(1, t).wait()

    @pl.when(ahead >= 2)
    def _():
        issue(1)

    for t in range(tiles):
        load(2, t).wait()
    for chunk in range(2, max(NEAR, FAR)):

        @pl.when(ahead > chunk)
        def _():
            issue(chunk)

    prepare()

    def edge(side):
        sent(side)
        if side == 0 and min(NEAR, FAR) == 1:

            @pl.when(ahead == 1)
            def _():
                issue(1)

            @pl.when(ahead > 1)
            def _():
                issue(ahead)

        else:
            issue(ahead + side)
        arrive(side)
        start = 0 if side == 0 else rows - 8

        def body(t, carry):
            frame_stage(t, start)
            for i in range(planes):
                outgoing[side, pl.ds((i * tiles + t) * 2, 2), :] = first[i, t, pl.ds(8 if side == 0 else rows + 6, 2), :]
            return carry

        lax.fori_loop(0, tiles, body, 0)

        @pl.when(has_upper if side == 0 else has_lower)
        def _():
            row_copy(side).start()

    edge(0)
    edge(1)

    def take(t):
        sent(t + 2)

        @pl.when(t + 2 + ahead < tiles + 2)
        def _():
            issue(t + 2 + ahead)

        arrive(t + 2)

        def body(step, carry):
            for j in range(2):
                frame_stage(t, pl.multiple_of(8 * (step * 2 + j + 1), 8))
            return carry

        lax.fori_loop(0, (groups - 2) // 2, body, 0)

    def early(t, carry):
        take(t)
        return carry

    lax.fori_loop(0, LATE + 1, early, 0)

    for side in range(2):
        place = rows + 8 if side == 0 else 6
        there = has_lower if side == 0 else has_upper

        @pl.when(there)
        def _():
            row_copy(side).wait_recv()

            def body(t, carry):
                for i in range(planes):
                    first[i, t, pl.ds(place, 2), :] = incoming[side, pl.ds((i * tiles + t) * 2, 2), :]
                return carry

            lax.fori_loop(0, tiles, body, 0)

        @pl.when(jnp.logical_not(there))
        def _():
            def body(t, carry):
                for i in range(planes):
                    first[i, t, pl.ds(place, 2), :] = jnp.zeros((2, LANES), jnp.float32)
                return carry

            lax.fori_loop(0, tiles, body, 0)

    row_stage(0)

    def catch_up(t, carry):
        row_stage(t + 1)
        finish(t)
        return carry

    lax.fori_loop(0, LATE, catch_up, 0)

    def late(t, carry):
        take(t)
        row_stage(t)
        finish(t - 1)
        return carry

    lax.fori_loop(LATE + 1, tiles - 1, late, 0)
    take(tiles - 1)

    for side in range(2):

        @pl.when(has_upper if side == 0 else has_lower)
        def _():
            row_copy(side).wait_send()


def moments_kernel(n_row, boxes, first, second_in, level, mix, weight_in, out, moments, second, weight, smooth, wide, parts, sem):
    depth, tiles, rows = weight.shape[0:3]
    slots = boxes.shape[1]

    def store(t):
        return pltpu.make_async_copy(weight.at[:, t], out.at[:, :, pl.ds(t * LANES, LANES)], sem.at[t])

    for t in range(tiles - 2):
        store(t).start()
    row_stage, finish = stages(n_row, first, second, smooth, wide, level, mix, weight)
    row_stage(tiles - 1)

    def tail(t, carry):
        finish(t)
        store(t).start()
        return carry

    lax.fori_loop(tiles - 2, tiles, tail, 0)
    frame_base = lax.axis_index("omega") * depth
    row_base = lax.axis_index("row") * rows
    sub = lax.broadcasted_iota(jnp.int32, (8, LANES), 0)
    lane = lax.broadcasted_iota(jnp.int32, (8, LANES), 1)
    half_f, half_r, half_c = ((BOX_F - 1) / 2.0, (BOX_R - 1) / 2.0, (BOX_C - 1) / 2.0)
    u_row = [((sub + 8 * j).astype(jnp.float32) - half_r) / half_r for j in range(2)]

    def box(b, carry):
        live = boxes[0, b] >= 0

        @pl.when(live)
        def _():
            f0 = boxes[0, b] - frame_base
            r0 = boxes[1, b] - row_base
            c0 = boxes[2, b]
            totals = None
            for side in range(2):
                tile = jnp.minimum(c0 // LANES + side, tiles - 1)
                distance = lane - (lax.rem(c0, LANES) - side * LANES)
                inside = (distance >= 0) & (distance < BOX_C)
                u_column = (distance.astype(jnp.float32) - half_c) / half_c
                plain = [None, None]
                framed = [None, None]
                for j in range(2):
                    for i in range(BOX_F):
                        w = weight[f0 + i, tile, pl.ds(r0 + 8 * j, 8), :]
                        m = w * ((i - half_f) / half_f)
                        plain[j] = w if i == 0 else plain[j] + w
                        framed[j] = m if i == 0 else framed[j] + m
                everything = plain[0] + plain[1]
                stats = [everything, framed[0] + framed[1], plain[0] * u_row[0] + plain[1] * u_row[1], everything * u_column]
                stats = [jnp.where(inside, s, 0.0) for s in stats]
                totals = stats if side == 0 else [p + q for p, q in zip(totals, stats)]
            for s in range(4):
                parts[s, pl.ds(pl.multiple_of(b * 8, 8), 8), :] = totals[s]

        @pl.when(jnp.logical_not(live))
        def _():
            for s in range(4):
                parts[s, pl.ds(pl.multiple_of(b * 8, 8), 8), :] = jnp.zeros((8, LANES), jnp.float32)

        return carry

    lax.fori_loop(0, slots, box, 0)
    ones = jnp.ones((8, LANES), jnp.float32)
    lines = []
    for s in range(4):
        total = parts[s, pl.ds(0, slots, stride=8), :]
        for j in range(1, 8):
            total = total + parts[s, pl.ds(j, slots, stride=8), :]
        sums = lax.dot_general(ones, total, (((1,), (1,)), ((), ())), precision=lax.Precision.HIGHEST, preferred_element_type=jnp.float32)
        lines.append(sums[0:1, :])
    moments[...] = jnp.concatenate(lines, axis=0) * (1.0 / (BOX_F * BOX_R * BOX_C))
    for t in range(tiles):
        store(t).wait()


def on_device(n_omega, n_row, frames, thresholds, spot_boxes):
    depth, rows, columns = frames.shape
    tiles = columns // LANES
    planes = depth + 2
    slots = spot_boxes.shape[1]
    vmem = functools.partial(pl.BlockSpec, memory_space=pltpu.VMEM)
    smem = functools.partial(pl.BlockSpec, memory_space=pltpu.SMEM)
    anywhere = functools.partial(pl.BlockSpec, memory_space=pl.ANY)
    tall = planes * (rows + 8)
    kept = (
        pltpu.VMEM((depth, tiles, rows, LANES), jnp.float32),
        pltpu.VMEM((planes, tiles, rows + 16, LANES), jnp.float32),
        pltpu.VMEM((tiles + 2, tall, LANES), jnp.float32),
        pltpu.VMEM((rows, LANES), jnp.float32),
        pltpu.VMEM((2 * LANES, 2 * LANES), jnp.bfloat16),
    )
    weight, first, second, level, mix = pl.pallas_call(
        functools.partial(spread_kernel, n_omega, n_row),
        out_shape=kept,
        in_specs=[pl.BlockSpec(memory_space=pltpu.HBM), pl.BlockSpec(memory_space=pltpu.HBM)],
        out_specs=tuple(vmem() for _ in kept),
        scratch_shapes=[
            pltpu.SMEM((rows,), jnp.int32),
            pltpu.VMEM((depth + 2 * REACH, tiles, rows, LANES), jnp.float32),
            pltpu.VMEM((tall, LANES), jnp.float32),
            pltpu.VMEM((tall, LANES), jnp.float32),
            pltpu.VMEM((2, planes * tiles * 2, LANES), jnp.float32),
            pltpu.VMEM((2, planes * tiles * 2, LANES), jnp.float32),
            pltpu.SemaphoreType.DMA,
            pltpu.SemaphoreType.DMA((3, tiles)),
            pltpu.SemaphoreType.DMA((2, tiles + 2)),
            pltpu.SemaphoreType.DMA((2, tiles + 2)),
            pltpu.SemaphoreType.DMA((2,)),
            pltpu.SemaphoreType.DMA((2,)),
        ],
        compiler_params=pltpu.CompilerParams(collective_id=0, has_side_effects=True, vmem_limit_bytes=40 << 20),
        name="spread",
    )(frames, thresholds)
    out = pl.pallas_call(
        functools.partial(moments_kernel, n_row),
        out_shape=(jax.ShapeDtypeStruct(frames.shape, jnp.float32), jax.ShapeDtypeStruct((4, slots), jnp.float32), kept[2], kept[0]),
        in_specs=[smem(), vmem(), vmem(), vmem(), vmem(), vmem()],
        out_specs=(anywhere(), vmem(), vmem(), vmem()),
        scratch_shapes=[
            pltpu.VMEM((tall, LANES), jnp.float32),
            pltpu.VMEM((tall, LANES), jnp.float32),
            pltpu.VMEM((4, slots * 8, LANES), jnp.float32),
            pltpu.SemaphoreType.DMA((tiles,)),
        ],
        input_output_aliases={2: 2, 5: 3},
        compiler_params=pltpu.CompilerParams(vmem_limit_bytes=8 << 20),
        name="moments",
    )(spot_boxes, first, second, level, mix, weight)
    return out[0:2]


def solution(mesh):
    return jax.shard_map(
        functools.partial(on_device, mesh.shape["omega"], mesh.shape["row"]),
        mesh=mesh,
        in_specs=(P("omega", "row", None), P("row"), P(None, ("omega", "row"))),
        out_specs=(P("omega", "row", None), P(None, ("omega", "row"))),
        check_vma=False,
    )
```

```python
import functools

import jax
import jax.numpy as jnp
from jax import lax
from jax.experimental import pallas as pl
from jax.experimental.pallas import tpu as pltpu
from jax.sharding import PartitionSpec as P

BW = 4
REACH = BW + 2
BOX_F = 8
BOX_R = 16
BOX_C = 16
SHARP = 8.0
LOG2E = 1.4426950408889634
BIG = 3.0e38
LANES = 128
NEAR, FAR = (3, 1)
LATE = 1
BLOCK = 18
ROW_STEP = 3
MESH = pl.DeviceIdType.MESH


def stages(n_row, first, second, smooth, wide, level, mix, weight):
    planes, tiles = (first.shape[0], first.shape[1])
    rows = level.shape[0]
    groups = rows // 8
    tall = rows + 8
    row = lax.axis_index("row")
    has_upper, has_lower = (row > 0, row < n_row - 1)

    def row_stage(t):
        def body(step, carry):
            for j in range(ROW_STEP):
                k = step * ROW_STEP + j
                for i in range(planes):
                    up = first[i, t, pl.ds(8 * k + 6, 8), :]
                    mid = first[i, t, pl.ds(8 * k + 7, 8), :]
                    down = first[i, t, pl.ds(8 * k + 8, 8), :]
                    second[t + 1, pl.ds(pl.multiple_of(i * tall + 8 * k, 8), 8), :] = (up + down) + (mid + mid)
            return carry

        lax.fori_loop(0, (groups + 1) // ROW_STEP, body, 0)

    def column_stage(t):
        size = (BLOCK * tall, LANES)
        lane = lax.broadcasted_iota(jnp.int32, size, 1)
        left_edge, right_edge = (lane == 0, lane == LANES - 1)
        left_half = lane >= LANES // 2
        low = jnp.where(t == 0, -BIG, BIG)
        high = jnp.where(t == tiles - 1, -BIG, BIG)
        bound = jnp.where(left_half, low, high)

        def body(m, carry):
            at = pl.ds(pl.multiple_of(m * (BLOCK * tall), 8), BLOCK * tall)
            middle = second[t + 1, at, :]
            whole = jnp.concatenate([middle, jnp.where(left_half, second[t, at, :], second[t + 2, at, :])], axis=1)
            upper = whole.astype(jnp.bfloat16)
            lower = (whole - upper.astype(jnp.float32)).astype(jnp.bfloat16)
            out = jnp.dot(upper, mix[...], preferred_element_type=jnp.float32) + jnp.dot(lower, mix[...], preferred_element_type=jnp.float32)
            value = out[:, 0:LANES]
            beside = jnp.minimum(out[:, LANES:], bound)
            from_left = pltpu.roll(jnp.where(right_edge, beside, value), 1, 1)
            from_right = pltpu.roll(jnp.where(left_edge, beside, value), LANES - 1, 1)
            wide[at, :] = jnp.maximum(jnp.maximum(from_left, from_right), value)
            smooth[at, :] = value
            return carry

        for m in range(planes // BLOCK):
            body(m, 0)

    def outside():
        @pl.when(jnp.logical_not(has_upper))
        def _():
            for i in range(planes):
                wide[i * tall : i * tall + 1, :] = jnp.full((1, LANES), -BIG)

        @pl.when(jnp.logical_not(has_lower))
        def _():
            for i in range(planes):
                wide[i * tall + rows + 1 : i * tall + rows + 2, :] = jnp.full((1, LANES), -BIG)

    def weight_stage(t):
        def group(g):
            start = pl.multiple_of(8 * g, 8)
            limit = level[pl.ds(start, 8), :]
            columns = []
            for i in range(planes):
                up = wide[pl.ds(i * tall + 8 * g, 8), :]
                mid = wide[pl.ds(i * tall + 8 * g + 1, 8), :]
                down = wide[pl.ds(i * tall + 8 * g + 2, 8), :]
                columns.append(jnp.maximum(jnp.maximum(up, down), mid))
                if i >= 2:
                    highest = jnp.maximum(jnp.maximum(columns[i - 2], columns[i - 1]), columns[i])
                    value = smooth[pl.ds((i - 1) * tall + 8 * g + 1, 8), :]
                    sharp = jnp.exp2((value - highest) * (SHARP * LOG2E / 64.0))
                    weight[i - 2, t, pl.ds(start, 8), :] = sharp * (jnp.maximum(value - limit, 0.0) * (1.0 / 64.0))

        def body(step, carry):
            for j in range(2):
                group(step * 2 + j)
            return carry

        lax.fori_loop(0, groups // 2, body, 0)

    def finish(t):
        column_stage(t)
        outside()
        weight_stage(t)

    return (row_stage, finish, column_stage, outside, weight_stage)


def spread_kernel(n_omega, n_row, frames, limits, weight, first, second, level, mix, thresholds, x, smooth, wide, outgoing, incoming, limit_sem, load_sem, send_sem, recv_sem, row_send, row_recv):
    depth, rows = (frames.shape[0], frames.shape[1])
    tiles = frames.shape[2] // LANES
    groups = rows // 8
    planes = depth + 2
    tall = rows + 8
    omega, row = (lax.axis_index("omega"), lax.axis_index("row"))
    after, before = (lax.rem(omega + 1, n_omega), lax.rem(omega + n_omega - 1, n_omega))
    has_upper, has_lower = (row > 0, row < n_row - 1)

    def load(part, t):
        start, count = ((0, 8), (rows - 8, 8), (8, rows - 16))[part]
        return pltpu.make_async_copy(
            frames.at[:, pl.ds(start, count), pl.ds(t * LANES, LANES)], x.at[pl.ds(REACH, depth), t, pl.ds(start, count), :], load_sem.at[part, t]
        )

    barrier = pltpu.get_barrier_semaphore()
    for neighbour in (before, after):
        pl.semaphore_signal(barrier, inc=1, device_id=(neighbour, row), device_id_type=MESH)

    @pl.when(has_upper)
    def _():
        pl.semaphore_signal(barrier, inc=1, device_id=(omega, row - 1), device_id_type=MESH)

    @pl.when(has_lower)
    def _():
        pl.semaphore_signal(barrier, inc=1, device_id=(omega, row + 1), device_id_type=MESH)

    limits_copy = pltpu.make_async_copy(limits, thresholds, limit_sem)
    for part in range(3):
        for t in range(tiles):
            load(part, t).start()
    limits_copy.start()

    sub = lax.broadcasted_iota(jnp.int32, (8, LANES), 0)

    def prepare():
        limits_copy.wait()
        for g in range(groups):
            tile = jnp.full((8, LANES), thresholds[g * 8].astype(jnp.float32))
            for j in range(1, 8):
                tile = jnp.where(sub == j, thresholds[g * 8 + j].astype(jnp.float32), tile)
            level[g * 8 : g * 8 + 8, :] = tile
        blank = jnp.zeros((tall, LANES), jnp.float32)
        for i in range(planes):
            second[0, i * tall : (i + 1) * tall, :] = blank
            second[tiles + 1, i * tall : (i + 1) * tall, :] = blank
        last = LANES - 1
        size = (LANES, LANES)
        source, place = (lax.broadcasted_iota(jnp.int32, size, 0), lax.broadcasted_iota(jnp.int32, size, 1))

        def taps(pairs):
            total = jnp.zeros(size, jnp.float32)
            for test, value in pairs:
                total = total + jnp.where(test, value, 0.0)
            return total.astype(jnp.bfloat16)

        at_first, at_last = (place == 0, place == last)
        mix[0:LANES, 0:LANES] = taps([(source == place, 2.0), (source == place - 1, 1.0), (source == place + 1, 1.0)])
        mix[LANES:, 0:LANES] = taps([(at_first & (source == last), 1.0), (at_last & (source == 0), 1.0)])
        mix[0:LANES, LANES:] = taps([(at_first & (source == last), 1.0), (at_last & (source == 0), 1.0)])
        mix[LANES:, LANES:] = taps(
            [(at_first & (source == 0), 2.0), (at_first & (source == 1), 1.0), (at_last & (source == last), 2.0), (at_last & (source == last - 1), 1.0)]
        )

    def piece(start, chunk):
        planes_of = pl.ds(start, REACH)
        if isinstance(chunk, int) and chunk < 2:
            return x.at[planes_of, :, pl.ds(0 if chunk == 0 else rows - 8, 8), :]
        return x.at[planes_of, chunk - 2, pl.ds(8, rows - 16), :]

    def copies(chunk):
        to_before = pltpu.make_async_remote_copy(
            src_ref=piece(REACH, chunk), dst_ref=piece(REACH + depth, chunk), send_sem=send_sem.at[0, chunk], recv_sem=recv_sem.at[0, chunk], device_id=(before, row), device_id_type=MESH
        )
        to_after = pltpu.make_async_remote_copy(
            src_ref=piece(depth, chunk), dst_ref=piece(0, chunk), send_sem=send_sem.at[1, chunk], recv_sem=recv_sem.at[1, chunk], device_id=(after, row), device_id_type=MESH
        )
        return (to_before, to_after)

    def row_copy(side):
        return pltpu.make_async_remote_copy(
            src_ref=outgoing.at[side], dst_ref=incoming.at[side], send_sem=row_send.at[side], recv_sem=row_recv.at[side], device_id=(omega, row - 1 if side == 0 else row + 1), device_id_type=MESH
        )

    for t in range(tiles):
        load(0, t).wait()
    pl.semaphore_wait(barrier, 2 + has_upper.astype(jnp.int32) + has_lower.astype(jnp.int32))

    def issue(chunk):
        for copy in copies(chunk):
            copy.start()

    corner = lax.rem(omega, 4)
    ahead = jnp.where((corner == 0) | (corner == 3), FAR, NEAR)

    def sent(chunk):
        for copy in copies(chunk):
            copy.wait_send()

    def arrive(chunk):
        for copy in copies(chunk):
            copy.wait_recv()

    def frame_stage(t, start):
        v = [x[j, t, pl.ds(start, 8), :] for j in range(depth + 2 * REACH)]
        s2 = [v[j] + v[j + 1] for j in range(len(v) - 1)]
        s4 = [s2[j] + s2[j + 2] for j in range(len(s2) - 2)]
        s8 = [s4[j] + s4[j + 4] for j in range(len(s4) - 4)]
        c = [v[j + BW] - (s8[j] + v[j + 2 * BW]) * (1.0 / (2 * BW + 1)) for j in range(depth + 4)]
        p = [c[j] + c[j + 1] for j in range(depth + 3)]
        for i in range(planes):
            first[i, t, pl.ds(start + 8, 8), :] = p[i] + p[i + 1]

    row_stage, finish = stages(n_row, first, second, smooth, wide, level, mix, weight)[0:2]

    issue(0)
    for t in range(tiles):
        load(1, t).wait()

    @pl.when(ahead >= 2)
    def _():
        issue(1)

    for t in range(tiles):
        load(2, t).wait()
    for chunk in range(2, max(NEAR, FAR)):

        @pl.when(ahead > chunk)
        def _():
            issue(chunk)

    prepare()

    def edge(side):
        sent(side)
        if side == 0 and min(NEAR, FAR) == 1:

            @pl.when(ahead == 1)
            def _():
                issue(1)

            @pl.when(ahead > 1)
            def _():
                issue(ahead)

        else:
            issue(ahead + side)
        arrive(side)
        start = 0 if side == 0 else rows - 8

        def body(t, carry):
            frame_stage(t, start)
            for i in range(planes):
                outgoing[side, pl.ds((i * tiles + t) * 2, 2), :] = first[i, t, pl.ds(8 if side == 0 else rows + 6, 2), :]
            return carry

        lax.fori_loop(0, tiles, body, 0)

        @pl.when(has_upper if side == 0 else has_lower)
        def _():
            row_copy(side).start()

    edge(0)
    edge(1)

    def take(t):
        sent(t + 2)

        @pl.when(t + 2 + ahead < tiles + 2)
        def _():
            issue(t + 2 + ahead)

        arrive(t + 2)

        def body(step, carry):
            for j in range(2):
                frame_stage(t, pl.multiple_of(8 * (step * 2 + j + 1), 8))
            return carry

        lax.fori_loop(0, (groups - 2) // 2, body, 0)

    def early(t, carry):
        take(t)
        return carry

    lax.fori_loop(0, LATE + 1, early, 0)

    for side in range(2):
        place = rows + 8 if side == 0 else 6
        there = has_lower if side == 0 else has_upper

        @pl.when(there)
        def _():
            row_copy(side).wait_recv()

            def body(t, carry):
                for i in range(planes):
                    first[i, t, pl.ds(place, 2), :] = incoming[side, pl.ds((i * tiles + t) * 2, 2), :]
                return carry

            lax.fori_loop(0, tiles, body, 0)

        @pl.when(jnp.logical_not(there))
        def _():
            def body(t, carry):
                for i in range(planes):
                    first[i, t, pl.ds(place, 2), :] = jnp.zeros((2, LANES), jnp.float32)
                return carry

            lax.fori_loop(0, tiles, body, 0)

    row_stage(0)

    def catch_up(t, carry):
        row_stage(t + 1)
        finish(t)
        return carry

    lax.fori_loop(0, LATE, catch_up, 0)

    def late(t, carry):
        take(t)
        row_stage(t)
        finish(t - 1)
        return carry

    lax.fori_loop(LATE + 1, tiles - 1, late, 0)
    take(tiles - 1)

    for side in range(2):

        @pl.when(has_upper if side == 0 else has_lower)
        def _():
            row_copy(side).wait_send()


def moments_kernel(n_row, boxes, first, second_in, level, mix, weight_in, out, moments, second, weight, smooth, wide, parts, sem):
    depth, tiles, rows = weight.shape[0:3]
    slots = boxes.shape[1]

    def store(t):
        return pltpu.make_async_copy(weight.at[:, t], out.at[:, :, pl.ds(t * LANES, LANES)], sem.at[t])

    for t in range(tiles - 2):
        store(t).start()
    row_stage = stages(n_row, first, second, smooth.at[0], wide.at[0], level, mix, weight)[0]
    row_stage(tiles - 1)

    ends = [stages(n_row, first, second, smooth.at[j], wide.at[j], level, mix, weight)[2:] for j in range(2)]
    for j in range(2):
        ends[j][0](tiles - 2 + j)
    for j in range(2):
        ends[j][1]()
        ends[j][2](tiles - 2 + j)
        store(tiles - 2 + j).start()
    frame_base = lax.axis_index("omega") * depth
    row_base = lax.axis_index("row") * rows
    sub = lax.broadcasted_iota(jnp.int32, (8, LANES), 0)
    lane = lax.broadcasted_iota(jnp.int32, (8, LANES), 1)
    half_f, half_r, half_c = ((BOX_F - 1) / 2.0, (BOX_R - 1) / 2.0, (BOX_C - 1) / 2.0)
    u_row = [((sub + 8 * j).astype(jnp.float32) - half_r) / half_r for j in range(2)]

    def box(b, carry):
        live = boxes[0, b] >= 0

        @pl.when(live)
        def _():
            f0 = boxes[0, b] - frame_base
            r0 = boxes[1, b] - row_base
            c0 = boxes[2, b]
            totals = None
            for side in range(2):
                tile = jnp.minimum(c0 // LANES + side, tiles - 1)
                distance = lane - (lax.rem(c0, LANES) - side * LANES)
                inside = (distance >= 0) & (distance < BOX_C)
                u_column = (distance.astype(jnp.float32) - half_c) / half_c
                plain = [None, None]
                framed = [None, None]
                for j in range(2):
                    for i in range(BOX_F):
                        w = weight[f0 + i, tile, pl.ds(r0 + 8 * j, 8), :]
                        m = w * ((i - half_f) / half_f)
                        plain[j] = w if i == 0 else plain[j] + w
                        framed[j] = m if i == 0 else framed[j] + m
                everything = plain[0] + plain[1]
                stats = [everything, framed[0] + framed[1], plain[0] * u_row[0] + plain[1] * u_row[1], everything * u_column]
                stats = [jnp.where(inside, s, 0.0) for s in stats]
                totals = stats if side == 0 else [p + q for p, q in zip(totals, stats)]
            for s in range(4):
                parts[s, pl.ds(pl.multiple_of(b * 8, 8), 8), :] = totals[s]

        @pl.when(jnp.logical_not(live))
        def _():
            for s in range(4):
                parts[s, pl.ds(pl.multiple_of(b * 8, 8), 8), :] = jnp.zeros((8, LANES), jnp.float32)

        return carry

    lax.fori_loop(0, slots, box, 0)
    ones = jnp.ones((8, LANES), jnp.float32)
    lines = []
    for s in range(4):
        total = parts[s, pl.ds(0, slots, stride=8), :]
        for j in range(1, 8):
            total = total + parts[s, pl.ds(j, slots, stride=8), :]
        sums = lax.dot_general(ones, total, (((1,), (1,)), ((), ())), precision=lax.Precision.HIGHEST, preferred_element_type=jnp.float32)
        lines.append(sums[0:1, :])
    moments[...] = jnp.concatenate(lines, axis=0) * (1.0 / (BOX_F * BOX_R * BOX_C))
    for t in range(tiles):
        store(t).wait()


def on_device(n_omega, n_row, frames, thresholds, spot_boxes):
    depth, rows, columns = frames.shape
    tiles = columns // LANES
    planes = depth + 2
    slots = spot_boxes.shape[1]
    vmem = functools.partial(pl.BlockSpec, memory_space=pltpu.VMEM)
    smem = functools.partial(pl.BlockSpec, memory_space=pltpu.SMEM)
    anywhere = functools.partial(pl.BlockSpec, memory_space=pl.ANY)
    tall = planes * (rows + 8)
    kept = (
        pltpu.VMEM((depth, tiles, rows, LANES), jnp.float32),
        pltpu.VMEM((planes, tiles, rows + 16, LANES), jnp.float32),
        pltpu.VMEM((tiles + 2, tall, LANES), jnp.float32),
        pltpu.VMEM((rows, LANES), jnp.float32),
        pltpu.VMEM((2 * LANES, 2 * LANES), jnp.bfloat16),
    )
    weight, first, second, level, mix = pl.pallas_call(
        functools.partial(spread_kernel, n_omega, n_row),
        out_shape=kept,
        in_specs=[pl.BlockSpec(memory_space=pltpu.HBM), pl.BlockSpec(memory_space=pltpu.HBM)],
        out_specs=tuple(vmem() for _ in kept),
        scratch_shapes=[
            pltpu.SMEM((rows,), jnp.int32),
            pltpu.VMEM((depth + 2 * REACH, tiles, rows, LANES), jnp.float32),
            pltpu.VMEM((tall, LANES), jnp.float32),
            pltpu.VMEM((tall, LANES), jnp.float32),
            pltpu.VMEM((2, planes * tiles * 2, LANES), jnp.float32),
            pltpu.VMEM((2, planes * tiles * 2, LANES), jnp.float32),
            pltpu.SemaphoreType.DMA,
            pltpu.SemaphoreType.DMA((3, tiles)),
            pltpu.SemaphoreType.DMA((2, tiles + 2)),
            pltpu.SemaphoreType.DMA((2, tiles + 2)),
            pltpu.SemaphoreType.DMA((2,)),
            pltpu.SemaphoreType.DMA((2,)),
        ],
        compiler_params=pltpu.CompilerParams(collective_id=0, has_side_effects=True, vmem_limit_bytes=40 << 20),
        name="spread",
    )(frames, thresholds)
    out = pl.pallas_call(
        functools.partial(moments_kernel, n_row),
        out_shape=(jax.ShapeDtypeStruct(frames.shape, jnp.float32), jax.ShapeDtypeStruct((4, slots), jnp.float32), kept[2], kept[0]),
        in_specs=[smem(), vmem(), vmem(), vmem(), vmem(), vmem()],
        out_specs=(anywhere(), vmem(), vmem(), vmem()),
        scratch_shapes=[
            pltpu.VMEM((2, tall, LANES), jnp.float32),
            pltpu.VMEM((2, tall, LANES), jnp.float32),
            pltpu.VMEM((4, slots * 8, LANES), jnp.float32),
            pltpu.SemaphoreType.DMA((tiles,)),
        ],
        input_output_aliases={2: 2, 5: 3},
        compiler_params=pltpu.CompilerParams(vmem_limit_bytes=8 << 20),
        name="moments",
    )(spot_boxes, first, second, level, mix, weight)
    return out[0:2]


def solution(mesh):
    return jax.shard_map(
        functools.partial(on_device, mesh.shape["omega"], mesh.shape["row"]),
        mesh=mesh,
        in_specs=(P("omega", "row", None), P("row"), P(None, ("omega", "row"))),
        out_specs=(P("omega", "row", None), P(None, ("omega", "row"))),
        check_vma=False,
    )
```
